32 devices in a mesh: south: 4 (over y, x), east: 2 (over core), down: 4 (over z).
Axes of the slice: x: 2, y: 2, z: 4, core: 2. Of those that a mesh axis runs over, the one named last changes fastest.
Arguments:
- field_now: float32 [32, 32, 512, 128], P('south', 'east', 'down'), may hold values from 0.2 to 1.8
- earlier: float32 [32, 32, 512, 128], P('south', 'east', 'down'), may hold values from 0.2 to 1.8
- speed_square: float32 [32, 32, 512, 128], P('south', 'east', 'down'), may hold values from 0.05 to 0.3
Outputs:
- running_total: float32 [32, 32, 512, 128], P('south', 'east', 'down')
- field_now_end: float32 [32, 32, 512, 128], P('south', 'east', 'down')
The draws below stay inside these ranges and needn't reach their ends.
All inputs are finite; a program needn't handle non-finite values.
Results may differ from the reference program's by a relative error of at most 0.00002.
Values sent between devices are 32-bit elements; how exact they have to be, the bound alone decides.
A program may use at most 320 MiB of HBM per device.

```python
import jax
import jax.numpy as jnp
from jax import lax

GRID_J = 32
GRID_I = 32
GRID_K = 512
MEMBERS = 128
STEPS = 4


def levels(stream_key, shape, cuts, smallest, largest):
    loudness = 1.0
    for dim, blocks in cuts:
        draws = jax.random.uniform(jax.random.fold_in(jax.random.fold_in(stream_key, 6), dim), (blocks,), jnp.float32, smallest / len(cuts), largest / len(cuts))
        loudness = loudness * jnp.repeat(jnp.exp(draws), shape[dim] // blocks).reshape((-1,) + (1,) * (len(shape) - 1 - dim))
    return loudness


def setup_inputs(seed: int = 0) -> dict:
    key_list = jax.random.split(jax.random.key(seed), 4)
    field_now = jnp.clip(0.2 + 1.5999999 * jax.random.uniform(key_list[0], (GRID_J, GRID_I, GRID_K, MEMBERS), jnp.float32) ** levels(key_list[0], (GRID_J, GRID_I, GRID_K, MEMBERS), ((0, 4), (1, 2), (2, 4)), -0.2, 0.2), 0.2, 1.8)
    earlier = jnp.clip(0.2 + 1.5999999 * jax.random.uniform(key_list[1], (GRID_J, GRID_I, GRID_K, MEMBERS), jnp.float32) ** levels(key_list[1], (GRID_J, GRID_I, GRID_K, MEMBERS), ((0, 4), (1, 2), (2, 4)), -0.2, 0.2), 0.2, 1.8)
    speed_square = jnp.clip(0.05 + 0.25 * jax.random.uniform(key_list[2], (GRID_J, GRID_I, GRID_K, MEMBERS), jnp.float32) ** levels(key_list[2], (GRID_J, GRID_I, GRID_K, MEMBERS), ((0, 4), (1, 2), (2, 4)), -0.2, 0.2), 0.05, 0.3)
    return {"field_now": field_now, "earlier": earlier, "speed_square": speed_square}


def strip_edges(values, dims):
    for dim in dims:
        values = lax.slice_in_dim(values, 1, values.shape[dim] - 1, axis=dim)
    return values


def neighbour(values, dim, start, dims):
    others = [other for other in dims if other != dim]
    values = strip_edges(values, others)
    return lax.slice_in_dim(values, start, start + values.shape[dim] - 2, axis=dim)


def one_step(padded, before, speed_square):
    middle = strip_edges(padded, (0, 1, 2))
    lower = [neighbour(padded, dim, 0, (0, 1, 2)) for dim in (0, 1, 2)]
    upper = [neighbour(padded, dim, 2, (0, 1, 2)) for dim in (0, 1, 2)]
    spread = lower[0] + upper[0] + lower[1] + upper[1] + lower[2] + upper[2] - 6.0 * middle
    return 2.0 * middle - before + speed_square * spread


def reference(field_now, earlier, speed_square):
    for step in range(STEPS):
        later = one_step(jnp.pad(field_now, ((1, 1), (1, 1), (1, 1), (0, 0)), mode="constant"), earlier, speed_square)
        earlier, field_now = field_now, later
    running_total = jnp.cumsum(field_now, axis=0) / GRID_J
    return running_total, field_now
```

```python
import functools

import jax
import jax.numpy as jnp
import numpy as np
from jax import lax
from jax.experimental import pallas as pl
from jax.experimental.pallas import tpu as pltpu
from jax.sharding import PartitionSpec as P

STEPS = 4
PIECES = 8
VMEM_LIMIT = 42 * 1024 * 1024
WRITER_LIMIT = 12 * 1024 * 1024
VIA = 1
MESH = pl.DeviceIdType.MESH


def corner_relays(mesh):
    devices = mesh.devices
    if not hasattr(devices.flat[0], "coords"):
        return {}
    south = devices.shape[list(mesh.axis_names).index("south")]
    lines = np.moveaxis(devices, list(mesh.axis_names).index("south"), 0).reshape(south, -1)
    found = {}
    for side, pairs in ((0, [(p, p - 1) for p in range(1, south)]),
                        (1, [(p, p + 1) for p in range(south - 1)])):
        for p, q in pairs:
            choices = set()
            for line in range(lines.shape[1]):
                a, b = lines[p, line].coords, lines[q, line].coords
                differ = [d for d in range(3) if a[d] != b[d]]
                if len(differ) != 2 or any(abs(a[d] - b[d]) != 1 for d in differ):
                    choices.add(None)
                    continue
                corner = list(a)
                corner[differ[VIA]] = b[differ[VIA]]
                at = [r for r in range(south) if list(lines[r, line].coords) == corner]
                choices.add(at[0] if at else None)
            if len(choices) == 1 and None not in choices:
                found[p, side] = choices.pop()
    fits = all(abs(r - (p - 1 if side == 0 else p + 1)) == 1 for (p, side), r in found.items())
    if len(set(found.values())) != len(found) or not fits:
        return {}
    return found


def kernel(
    sizes, relays, u_hbm, e_hbm, c_hbm, c, end, before,
    ab, z, zs, pin, sbuf,
    s_send, s_recv, d_send, d_recv, e_send, e_recv,
    ei_send, ei_recv, di_send, di_recv, p_send, p_recv, load_sem, *hops,
):
    rows, cols, depth, lanes = u_hbm.shape
    pieces = min(PIECES, cols)
    wide = cols // pieces
    place = {axis: lax.axis_index(axis) for axis in sizes}
    below = {axis: place[axis] > 0 for axis in sizes}
    above = {axis: place[axis] < sizes[axis] - 1 for axis in sizes}
    scale = 1.0 / (rows * sizes["south"])

    odd = lax.rem(place["east"], 2) == 1

    def piece(n):
        return jnp.where(odd, n, pieces - 1 - n)

    def target(axis, side):
        step = sizes[axis] - 1 if side == 0 else 1
        return {axis: lax.rem(place[axis] + step, sizes[axis])}

    def sends(axis, side):
        return below[axis] if side == 0 else above[axis]

    def receives(axis, side):
        return above[axis] if side == 0 else below[axis]

    def remote(src, dst, send, recv, axis, side):
        return pltpu.make_async_remote_copy(
            src_ref=src, dst_ref=dst, send_sem=send, recv_sem=recv,
            device_id=target(axis, side), device_id_type=MESH,
        )

    def south(slot, side, n, first=False):
        here = (1, rows)[side]
        there = (rows + 1, 0)[side]
        src = (
            u_hbm.at[here - 1, pl.ds(n * wide, wide)]
            if first else ab.at[slot, here, pl.ds(n * wide + 1, wide)]
        )
        return remote(
            src, ab.at[slot, there, pl.ds(n * wide + 1, wide)],
            s_send.at[slot, side, n], s_recv.at[slot, side, n], "south", side,
        )

    def down(slot, side, n):
        part = (pl.ds(0, 2), pl.ds(n * wide, wide))
        return remote(
            zs.at[(slot, side) + part], z.at[(slot, 1 - side) + part],
            d_send.at[slot, side, n], d_recv.at[slot, side, n], "down", side,
        )

    def down_inner(slot, side):
        part = pl.ds(2, rows - 2)
        return remote(
            zs.at[slot, side, part], z.at[slot, 1 - side, part],
            di_send.at[slot, side], di_recv.at[slot, side], "down", side,
        )

    def east(slot, side, k, first=False):
        here = (1, cols)[side]
        there = (cols + 1, 0)[side]
        row = (1, rows)[k]
        src = u_hbm.at[row - 1, here - 1] if first else ab.at[slot, row, here]
        return remote(
            src, ab.at[slot, row, there],
            e_send.at[slot, side, k], e_recv.at[slot, side, k], "east", side,
        )

    def east_inner(slot, side, first=False):
        here = (1, cols)[side]
        there = (cols + 1, 0)[side]
        src = (
            u_hbm.at[pl.ds(1, rows - 2), here - 1]
            if first else ab.at[slot, pl.ds(2, rows - 2), here]
        )
        return remote(
            src, ab.at[slot, pl.ds(2, rows - 2), there],
            ei_send.at[slot, side], ei_recv.at[slot, side], "east", side,
        )

    square = False
    if relays:
        relay_buf, h_recv, h_send, held, q_send, q_recv = hops
    square = sizes["south"] == 4 and relays == {(2, 0): 0, (1, 1): 3}

    def by_place(table, other):
        value = jnp.int32(other)
        for p, entry in table.items():
            value = jnp.where(place["south"] == p, entry, value)
        return value

    relay_at = [
        by_place({p: r for (p, s), r in relays.items() if s == side}, -1) for side in (0, 1)
    ]
    served = by_place({r: p for (p, _), r in relays.items()}, -1)
    served_side = by_place({r: side for (_, side), r in relays.items()}, 0)
    is_relay = served >= 0

    def hop_in(t, slot, side, n, m, first=False):
        here = (1, rows)[side]
        src = (
            u_hbm.at[here - 1, pl.ds(n * wide, wide)]
            if first else ab.at[slot, here, pl.ds(n * wide + 1, wide)]
        )
        return pltpu.make_async_remote_copy(
            src_ref=src, dst_ref=relay_buf.at[t, m],
            send_sem=s_send.at[slot, side, n], recv_sem=h_recv.at[t, m],
            device_id={"south": jnp.maximum(relay_at[side], 0)}, device_id_type=MESH,
        )

    def hop_out(t, m):
        n = piece(2 * m + 1)
        slot = lax.rem(jnp.int32(t), 2)
        there = jnp.where(served_side == 0, rows + 1, 0)
        goal = served + 2 * served_side - 1
        return pltpu.make_async_remote_copy(
            src_ref=relay_buf.at[t, m],
            dst_ref=ab.at[slot, there, pl.ds(n * wide + 1, wide)],
            send_sem=h_send.at[t, m], recv_sem=s_recv.at[slot, served_side, n],
            device_id={"south": jnp.maximum(goal, 0)}, device_id_type=MESH,
        )

    def forward(t, m):
        if relays:
            @pl.when(is_relay)
            def _():
                hop_in(t, 0, 0, 0, m).wait_recv()
                hop_out(t, m).start()

    def send_south(t, slot, turn, first=False):
        n = piece(turn)
        for side in (0, 1):
            here = sends("south", side)
            if relays:
                bent = jnp.logical_and(relay_at[side] >= 0, lax.rem(turn, 2) == 1)

                @pl.when(jnp.logical_and(here, bent))
                def _():
                    hop_in(t, slot, side, n, turn // 2, first).start()

                here = jnp.logical_and(here, jnp.logical_not(bent))

            @pl.when(here)
            def _():
                south(slot, side, n, first).start()

    def each(act, when, axis, copy):
        for side in (0, 1):
            @pl.when(when(axis, side))
            def _():
                getattr(copy(side), act)()

    barrier = pltpu.get_barrier_semaphore()
    for axis in sizes:
        for side in (0, 1):
            @pl.when(sends(axis, side))
            def _():
                pl.semaphore_signal(
                    barrier, inc=1, device_id=target(axis, side), device_id_type=MESH
                )
    met = 0
    if relays:
        for side in (0, 1):
            @pl.when(relay_at[side] >= 0)
            def _():
                pl.semaphore_signal(
                    barrier, inc=1, device_id={"south": jnp.maximum(relay_at[side], 0)},
                    device_id_type=MESH,
                )

            met = met + (relay_at[side] >= 0).astype(jnp.int32)

        @pl.when(is_relay)
        def _():
            pl.semaphore_signal(
                barrier, inc=1, device_id={"south": jnp.maximum(served, 0)},
                device_id_type=MESH,
            )

        met = met + is_relay.astype(jnp.int32)
    for axis in sizes:
        met = met + below[axis].astype(jnp.int32) + above[axis].astype(jnp.int32)

    own = (pl.ds(1, rows), pl.ds(1, cols))
    loads = [
        pltpu.make_async_copy(u_hbm, ab.at[(0,) + own], load_sem.at[0]),
        pltpu.make_async_copy(e_hbm, ab.at[(1,) + own], load_sem.at[1]),
        pltpu.make_async_copy(c_hbm, c, load_sem.at[2]),
    ]
    loads[0].start()
    pl.semaphore_wait(barrier, met)

    @pl.loop(0, pieces)
    def _(n):
        send_south(0, 0, n, True)

    for k in (0, 1):
        each("start", sends, "east", lambda side: east(0, side, k, True))
    each("start", sends, "east", lambda side: east_inner(0, side, True))
    loads[1].start()
    loads[2].start()

    blank = jnp.zeros((depth, lanes), jnp.float32)
    for side, missing in ((0, below), (1, above)):
        @pl.when(jnp.logical_not(missing["south"]))
        def _():
            @pl.loop(0, cols)
            def _(i):
                for slot in (0, 1):
                    ab[slot, (0, rows + 1)[side], i + 1] = blank

        @pl.when(jnp.logical_not(missing["east"]))
        def _():
            @pl.loop(0, rows)
            def _(j):
                for slot in (0, 1):
                    ab[slot, j + 1, (0, cols + 1)[side]] = blank

        @pl.when(jnp.logical_not(missing["down"]))
        def _():
            @pl.loop(0, cols)
            def _(i):
                for slot in (0, 1):
                    for r in range(rows):
                        z[slot, side, r, i] = blank[:1]

    loads[0].wait()

    @pl.loop(0, cols)
    def _(i):
        for r in range(rows):
            j = 0 if r == 0 else rows - 1 if r == 1 else r - 1
            zs[0, 0, r, i] = ab[0, j + 1, i + 1, pl.ds(0, 1)]
            zs[0, 1, r, i] = ab[0, j + 1, i + 1, pl.ds(depth - 1, 1)]

    @pl.loop(0, pieces)
    def _(n):
        each("start", sends, "down", lambda side: down(0, side, piece(n)))

    each("start", sends, "down", lambda side: down_inner(0, side))
    loads[1].wait()
    loads[2].wait()

    for m in range(pieces // 2):
        forward(0, m)

    level = lax.broadcasted_iota(jnp.int32, (depth, lanes), 0)

    def cell(now, later, j, i, r, final=False):
        x = ab[now, j + 1, i + 1]
        lower = jnp.where(level == 0, z[now, 0, r, i], pltpu.roll(x, 1, 0))
        upper = jnp.where(level == depth - 1, z[now, 1, r, i], pltpu.roll(x, depth - 1, 0))
        spread = (
            ab[now, j, i + 1] + ab[now, j + 2, i + 1]
            + ab[now, j + 1, i] + ab[now, j + 1, i + 2]
            + lower + upper - 6.0 * x
        )
        new = 2.0 * x - ab[later, j + 1, i + 1] + c[j, i] * spread
        if final:
            end[j, i] = new
            return
        ab[later, j + 1, i + 1] = new
        zs[later, 0, r, i] = new[:1]
        zs[later, 1, r, i] = new[depth - 1:]

    def inner(step, now, later, final=False):
        each("wait_recv", receives, "east", lambda side: east_inner(now, side))
        each("wait_recv", receives, "down", lambda side: down_inner(now, side))

        @pl.when(step >= 1)
        def _():
            each("wait_send", sends, "east", lambda side: east_inner(later, side))
            each("wait_send", sends, "down", lambda side: down_inner(later, side))

        @pl.loop(1, rows - 1)
        def _(j):
            @pl.loop(0, cols)
            def _(i):
                cell(now, later, j, i, j + 1, final)

        @pl.when(step < STEPS - 1)
        def _():
            each("start", sends, "east", lambda side: east_inner(later, side))
            each("start", sends, "down", lambda side: down_inner(later, side))

    def outer_edges(act, when, slot, n):
        for side in (0, 1):
            end = (0, pieces - 1)[side if when is sends else 1 - side]

            @pl.when(jnp.logical_and(when("east", side), n == end))
            def _():
                for k in (0, 1):
                    getattr(east(slot, side, k), act)()

    def outer_piece(step, now, later, turn, final=False):
        n = piece(turn)
        each("wait_recv", receives, "south", lambda side: south(now, side, n))
        each("wait_recv", receives, "down", lambda side: down(now, side, n))
        outer_edges("wait_recv", receives, now, n)

        @pl.when(step >= 1)
        def _():
            each("wait_send", sends, "south", lambda side: south(later, side, n))
            each("wait_send", sends, "down", lambda side: down(later, side, n))
            outer_edges("wait_send", sends, later, n)

        @pl.loop(0, wide)
        def _(w):
            i = n * wide + w
            cell(now, later, 0, i, 0, final)
            cell(now, later, rows - 1, i, 1, final)

        @pl.when(step < STEPS - 1)
        def _():
            send_south(step + 1, later, turn)
            each("start", sends, "down", lambda side: down(later, side, n))
            outer_edges("start", sends, later, n)

    @pl.loop(0, STEPS - 1)
    def _(step):
        now = lax.rem(step, 2)
        inner(step, now, 1 - now)

        @pl.loop(0, pieces)
        def _(n):
            outer_piece(step, now, 1 - now, n)
            if relays:
                @pl.when(jnp.logical_and(lax.rem(n, 2) == 1, n >= 3))
                def _():
                    forward(step + 1, n // 2 - 1)

        if relays:
            forward(step + 1, pieces // 2 - 1)

    last = STEPS - 1
    now, later = last % 2, 1 - last % 2
    inner(last, now, later, True)

    def carry(n):
        return remote(
            sbuf.at[pl.ds(n * wide, wide)], pin.at[pl.ds(n * wide, wide)],
            p_send.at[n], p_recv.at[n], "south", 1,
        )

    first = jnp.logical_not(below["south"])
    spot = place["south"]

    def total_copy(n, src, dst, way, kind, goal):
        part = pl.ds(n * wide, wide)
        return pltpu.make_async_remote_copy(
            src_ref=src.at[part], dst_ref=dst.at[part],
            send_sem=q_send.at[way, n], recv_sem=q_recv.at[kind, n],
            device_id={"south": goal}, device_id_type=MESH,
        )

    def beside(n):
        return total_copy(n, sbuf, pin, 0, 0, lax.rem(spot + 1, 4))

    def across(n):
        return total_copy(n, sbuf, pin, 1, 0, 2)

    def upward(n):
        return total_copy(n, sbuf, held, 1, 1, 3)

    def onward(n):
        return total_copy(n, held, held, 1, 1, 2)

    def middle_total(turn):
        n = piece(turn)

        @pl.when(spot == 2)
        def _():
            beside(n).wait_recv()

            @pl.loop(0, wide)
            def _(w):
                i = n * wide + w
                sbuf[i] = pin[i] + c[rows - 1, i]

            beside(n).start()

        @pl.when(spot == 3)
        def _():
            upward(n).wait_recv()
            onward(n).start()

    @pl.loop(0, pieces)
    def _(turn):
        n = piece(turn)
        outer_piece(last, now, later, turn, True)

        @pl.loop(0, wide)
        def _(w):
            i = n * wide + w
            sum_here = jnp.zeros((depth, lanes), jnp.float32)
            for j in range(rows):
                sum_here = sum_here + end[j, i]
                c[j, i] = sum_here * scale

        if square:
            @pl.when(spot < 2)
            def _():
                @pl.loop(0, wide)
                def _(w):
                    i = n * wide + w
                    sbuf[i] = c[rows - 1, i]

            @pl.when(spot == 0)
            def _():
                beside(n).start()
                across(n).start()

            @pl.when(spot == 1)
            def _():
                upward(n).start()

            @pl.when(turn >= 2)
            def _():
                middle_total(turn - 2)
        else:
            @pl.when(first)
            def _():
                @pl.loop(0, wide)
                def _(w):
                    i = n * wide + w
                    sbuf[i] = c[rows - 1, i]

                @pl.when(above["south"])
                def _():
                    carry(n).start()

    @pl.when(first)
    def _():
        @pl.loop(0, cols)
        def _(i):
            before[i] = blank

    if square:
        @pl.loop(pieces - 2, pieces)
        def _(turn):
            middle_total(turn)

        @pl.when(spot == 1)
        def _():
            @pl.loop(0, pieces)
            def _(turn):
                n = piece(turn)
                beside(n).wait_recv()

                @pl.loop(0, wide)
                def _(w):
                    i = n * wide + w
                    before[i] = pin[i]

        @pl.when(spot >= 2)
        def _():
            @pl.loop(0, pieces)
            def _(turn):
                n = piece(turn)

                @pl.when(spot == 2)
                def _():
                    upward(n).wait_recv()

                @pl.when(spot == 3)
                def _():
                    beside(n).wait_recv()

                @pl.loop(0, wide)
                def _(w):
                    i = n * wide + w
                    before[i] = pin[i] + held[i]
    else:
        @pl.when(below["south"])
        def _():
            @pl.loop(0, pieces)
            def _(turn):
                n = piece(turn)
                carry(n).wait_recv()

                @pl.loop(0, wide)
                def _(w):
                    i = n * wide + w
                    sbuf[i] = c[rows - 1, i] + pin[i]
                    before[i] = pin[i]

                @pl.when(above["south"])
                def _():
                    carry(n).start()

    if relays:
        @pl.when(is_relay)
        def _():
            for t in range(STEPS):
                for m in range(pieces // 2):
                    hop_out(t, m).wait_send()

    each("wait_send", sends, "east", lambda side: east_inner(now, side))
    each("wait_send", sends, "down", lambda side: down_inner(now, side))
    for k in (0, 1):
        each("wait_send", sends, "east", lambda side: east(now, side, k))

    @pl.loop(0, pieces)
    def _(n):
        each("wait_send", sends, "south", lambda side: south(now, side, n))
        each("wait_send", sends, "down", lambda side: down(now, side, n))

        if square:
            @pl.when(lax.rem(spot, 2) == 0)
            def _():
                beside(n).wait_send()

            @pl.when(spot != 2)
            def _():
                across(n).wait_send()
        else:
            @pl.when(above["south"])
            def _():
                carry(n).wait_send()


def writer(part, end, before, total_hbm, end_hbm, total, t_sem, e_sem):
    rows, cols = part.shape[:2]
    ends = [pltpu.make_async_copy(end.at[j], end_hbm.at[j], e_sem.at[j]) for j in range(rows)]
    totals = [
        pltpu.make_async_copy(total.at[j], total_hbm.at[j], t_sem.at[j]) for j in range(rows)
    ]
    for copy in ends:
        copy.start()
    for j in range(rows):
        @pl.loop(0, cols)
        def _(i):
            total[j, i] = part[j, i] + before[i]

        totals[j].start()
    for copy in ends + totals:
        copy.wait()


def shards(sizes, relays, field_now, earlier, speed_square):
    rows, cols, depth, lanes = field_now.shape
    pieces = min(PIECES, cols)
    relays = relays if pieces % 2 == 0 else {}
    edge = (2, 2, rows, cols, 1, lanes)
    dma = pltpu.SemaphoreType.DMA
    anywhere = pl.BlockSpec(memory_space=pltpu.HBM)
    inside = pl.BlockSpec(memory_space=pltpu.VMEM)
    part, end, before = pl.pallas_call(
        functools.partial(kernel, sizes, relays),
        out_shape=(
            pltpu.VMEM(field_now.shape, jnp.float32),
            pltpu.VMEM(field_now.shape, jnp.float32),
            pltpu.VMEM((cols, depth, lanes), jnp.float32),
        ),
        in_specs=[anywhere] * 3,
        out_specs=(inside,) * 3,
        scratch_shapes=[
            pltpu.VMEM((2, rows + 2, cols + 2, depth, lanes), jnp.float32),
            pltpu.VMEM(edge, jnp.float32),
            pltpu.VMEM(edge, jnp.float32),
            pltpu.VMEM((cols, depth, lanes), jnp.float32),
            pltpu.VMEM((cols, depth, lanes), jnp.float32),
            dma((2, 2, pieces)), dma((2, 2, pieces)),
            dma((2, 2, pieces)), dma((2, 2, pieces)),
            dma((2, 2, 2)), dma((2, 2, 2)),
            dma((2, 2)), dma((2, 2)), dma((2, 2)), dma((2, 2)),
            dma((pieces,)), dma((pieces,)), dma((3,)),
        ] + ([
            pltpu.VMEM((STEPS, pieces // 2, cols // pieces, depth, lanes), jnp.float32),
            dma((STEPS, pieces // 2)), dma((STEPS, pieces // 2)),
            pltpu.VMEM((cols, depth, lanes), jnp.float32),
            dma((2, pieces)), dma((2, pieces)),
        ] if relays else []),
        compiler_params=pltpu.CompilerParams(
            collective_id=0, has_side_effects=True, vmem_limit_bytes=VMEM_LIMIT
        ),
        name="wave",
    )(field_now, earlier, speed_square)
    return pl.pallas_call(
        writer,
        out_shape=(jax.ShapeDtypeStruct(field_now.shape, jnp.float32),) * 2,
        in_specs=[inside] * 3,
        out_specs=(anywhere,) * 2,
        scratch_shapes=[pltpu.VMEM(field_now.shape, jnp.float32), dma((rows,)), dma((rows,))],
        compiler_params=pltpu.CompilerParams(vmem_limit_bytes=WRITER_LIMIT),
        name="write",
    )(part, end, before)


def solution(mesh):
    placed = P("south", "east", "down", None)
    sizes = {axis: mesh.shape[axis] for axis in ("south", "east", "down")}
    relays = corner_relays(mesh)
    return jax.shard_map(
        functools.partial(shards, sizes, relays),
        mesh=mesh,
        in_specs=(placed,) * 3,
        out_specs=(placed,) * 2,
        check_vma=False,
    )
```

```python
import functools

import jax
import jax.numpy as jnp
import numpy as np
from jax import lax
from jax.experimental import pallas as pl
from jax.experimental.pallas import tpu as pltpu
from jax.sharding import PartitionSpec as P

STEPS = 4
PIECES = 8
VMEM_LIMIT = 42 * 1024 * 1024
WRITER_LIMIT = 12 * 1024 * 1024
VIA = 1
MESH = pl.DeviceIdType.MESH


def corner_relays(mesh):
    devices = mesh.devices
    if not hasattr(devices.flat[0], "coords"):
        return {}
    south = devices.shape[list(mesh.axis_names).index("south")]
    lines = np.moveaxis(devices, list(mesh.axis_names).index("south"), 0).reshape(south, -1)
    found = {}
    for side, pairs in ((0, [(p, p - 1) for p in range(1, south)]),
                        (1, [(p, p + 1) for p in range(south - 1)])):
        for p, q in pairs:
            choices = set()
            for line in range(lines.shape[1]):
                a, b = lines[p, line].coords, lines[q, line].coords
                differ = [d for d in range(3) if a[d] != b[d]]
                if len(differ) != 2 or any(abs(a[d] - b[d]) != 1 for d in differ):
                    choices.add(None)
                    continue
                corner = list(a)
                corner[differ[VIA]] = b[differ[VIA]]
                at = [r for r in range(south) if list(lines[r, line].coords) == corner]
                choices.add(at[0] if at else None)
            if len(choices) == 1 and None not in choices:
                found[p, side] = choices.pop()
    fits = all(abs(r - (p - 1 if side == 0 else p + 1)) == 1 for (p, side), r in found.items())
    if len(set(found.values())) != len(found) or not fits:
        return {}
    return found


def kernel(
    sizes, relays, u_hbm, e_hbm, c_hbm, c, end, before,
    ab, z, zs, pin, sbuf,
    s_send, s_recv, d_send, d_recv, e_send, e_recv,
    ei_send, ei_recv, di_send, di_recv, p_send, p_recv, load_sem, *hops,
):
    rows, cols, depth, lanes = u_hbm.shape
    pieces = min(PIECES, cols)
    wide = cols // pieces
    place = {axis: lax.axis_index(axis) for axis in sizes}
    below = {axis: place[axis] > 0 for axis in sizes}
    above = {axis: place[axis] < sizes[axis] - 1 for axis in sizes}
    scale = 1.0 / (rows * sizes["south"])

    odd = lax.rem(place["east"], 2) == 1

    def piece(n):
        return jnp.where(odd, n, pieces - 1 - n)

    def target(axis, side):
        step = sizes[axis] - 1 if side == 0 else 1
        return {axis: lax.rem(place[axis] + step, sizes[axis])}

    def sends(axis, side):
        return below[axis] if side == 0 else above[axis]

    def receives(axis, side):
        return above[axis] if side == 0 else below[axis]

    def remote(src, dst, send, recv, axis, side):
        return pltpu.make_async_remote_copy(
            src_ref=src, dst_ref=dst, send_sem=send, recv_sem=recv,
            device_id=target(axis, side), device_id_type=MESH,
        )

    def south(slot, side, n):
        here = (1, rows)[side]
        there = (rows + 1, 0)[side]
        return remote(
            ab.at[slot, here, pl.ds(n * wide + 1, wide)],
            ab.at[slot, there, pl.ds(n * wide + 1, wide)],
            s_send.at[slot, side, n], s_recv.at[slot, side, n], "south", side,
        )

    def down(slot, side, n):
        part = (pl.ds(0, 2), pl.ds(n * wide, wide))
        return remote(
            zs.at[(slot, side) + part], z.at[(slot, 1 - side) + part],
            d_send.at[slot, side, n], d_recv.at[slot, side, n], "down", side,
        )

    def down_inner(slot, side):
        part = pl.ds(2, rows - 2)
        return remote(
            zs.at[slot, side, part], z.at[slot, 1 - side, part],
            di_send.at[slot, side], di_recv.at[slot, side], "down", side,
        )

    def east(slot, side, k, first=False):
        here = (1, cols)[side]
        there = (cols + 1, 0)[side]
        row = (1, rows)[k]
        src = u_hbm.at[row - 1, here - 1] if first else ab.at[slot, row, here]
        return remote(
            src, ab.at[slot, row, there],
            e_send.at[slot, side, k], e_recv.at[slot, side, k], "east", side,
        )

    def east_inner(slot, side, first=False):
        here = (1, cols)[side]
        there = (cols + 1, 0)[side]
        src = (
            u_hbm.at[pl.ds(1, rows - 2), here - 1]
            if first else ab.at[slot, pl.ds(2, rows - 2), here]
        )
        return remote(
            src, ab.at[slot, pl.ds(2, rows - 2), there],
            ei_send.at[slot, side], ei_recv.at[slot, side], "east", side,
        )

    square = False
    if relays:
        relay_buf, h_recv, h_send, held, q_send, q_recv = hops
    square = sizes["south"] == 4 and relays == {(2, 0): 0, (1, 1): 3}

    def by_place(table, other):
        value = jnp.int32(other)
        for p, entry in table.items():
            value = jnp.where(place["south"] == p, entry, value)
        return value

    relay_at = [
        by_place({p: r for (p, s), r in relays.items() if s == side}, -1) for side in (0, 1)
    ]
    served = by_place({r: p for (p, _), r in relays.items()}, -1)
    served_side = by_place({r: side for (_, side), r in relays.items()}, 0)
    is_relay = served >= 0

    def hop_in(t, slot, side, n, m):
        here = (1, rows)[side]
        return pltpu.make_async_remote_copy(
            src_ref=ab.at[slot, here, pl.ds(n * wide + 1, wide)],
            dst_ref=relay_buf.at[t, m],
            send_sem=s_send.at[slot, side, n], recv_sem=h_recv.at[t, m],
            device_id={"south": jnp.maximum(relay_at[side], 0)}, device_id_type=MESH,
        )

    def hop_out(t, m):
        n = piece(2 * m + 1)
        slot = lax.rem(jnp.int32(t), 2)
        there = jnp.where(served_side == 0, rows + 1, 0)
        goal = served + 2 * served_side - 1
        return pltpu.make_async_remote_copy(
            src_ref=relay_buf.at[t, m],
            dst_ref=ab.at[slot, there, pl.ds(n * wide + 1, wide)],
            send_sem=h_send.at[t, m], recv_sem=s_recv.at[slot, served_side, n],
            device_id={"south": jnp.maximum(goal, 0)}, device_id_type=MESH,
        )

    def forward(t, m):
        if relays:
            @pl.when(is_relay)
            def _():
                hop_in(t, 0, 0, 0, m).wait_recv()
                hop_out(t, m).start()

    def send_south(t, slot, turn):
        n = piece(turn)
        for side in (0, 1):
            here = sends("south", side)
            if relays:
                bent = jnp.logical_and(relay_at[side] >= 0, lax.rem(turn, 2) == 1)

                @pl.when(jnp.logical_and(here, bent))
                def _():
                    hop_in(t, slot, side, n, turn // 2).start()

                here = jnp.logical_and(here, jnp.logical_not(bent))

            @pl.when(here)
            def _():
                south(slot, side, n).start()

    def each(act, when, axis, copy):
        for side in (0, 1):
            @pl.when(when(axis, side))
            def _():
                getattr(copy(side), act)()

    def row_load(first, count, sem):
        return pltpu.make_async_copy(
            u_hbm.at[pl.ds(first, count)],
            ab.at[0, pl.ds(first + 1, count), pl.ds(1, cols)], load_sem.at[sem],
        )

    edge_loads = [row_load(0, 1, 3), row_load(rows - 1, 1, 4)]
    loads = [
        row_load(1, rows - 2, 0),
        pltpu.make_async_copy(
            e_hbm, ab.at[1, pl.ds(1, rows), pl.ds(1, cols)], load_sem.at[1]
        ),
        pltpu.make_async_copy(c_hbm, c, load_sem.at[2]),
    ]
    for copy in edge_loads + loads[:1]:
        copy.start()

    barrier = pltpu.get_barrier_semaphore()
    for axis in sizes:
        for side in (0, 1):
            @pl.when(sends(axis, side))
            def _():
                pl.semaphore_signal(
                    barrier, inc=1, device_id=target(axis, side), device_id_type=MESH
                )
    met = 0
    if relays:
        for side in (0, 1):
            @pl.when(relay_at[side] >= 0)
            def _():
                pl.semaphore_signal(
                    barrier, inc=1, device_id={"south": jnp.maximum(relay_at[side], 0)},
                    device_id_type=MESH,
                )

            met = met + (relay_at[side] >= 0).astype(jnp.int32)

        @pl.when(is_relay)
        def _():
            pl.semaphore_signal(
                barrier, inc=1, device_id={"south": jnp.maximum(served, 0)},
                device_id_type=MESH,
            )

        met = met + is_relay.astype(jnp.int32)
    for axis in sizes:
        met = met + below[axis].astype(jnp.int32) + above[axis].astype(jnp.int32)

    pl.semaphore_wait(barrier, met)
    for copy in edge_loads:
        copy.wait()

    @pl.loop(0, pieces)
    def _(n):
        send_south(0, 0, n)

    for k in (0, 1):
        each("start", sends, "east", lambda side: east(0, side, k, True))
    each("start", sends, "east", lambda side: east_inner(0, side, True))
    loads[1].start()
    loads[2].start()

    blank = jnp.zeros((depth, lanes), jnp.float32)
    for side, missing in ((0, below), (1, above)):
        @pl.when(jnp.logical_not(missing["south"]))
        def _():
            @pl.loop(0, cols)
            def _(i):
                for slot in (0, 1):
                    ab[slot, (0, rows + 1)[side], i + 1] = blank

        @pl.when(jnp.logical_not(missing["east"]))
        def _():
            @pl.loop(0, rows)
            def _(j):
                for slot in (0, 1):
                    ab[slot, j + 1, (0, cols + 1)[side]] = blank

        @pl.when(jnp.logical_not(missing["down"]))
        def _():
            @pl.loop(0, cols)
            def _(i):
                for slot in (0, 1):
                    for r in range(rows):
                        z[slot, side, r, i] = blank[:1]

    loads[0].wait()

    @pl.loop(0, cols)
    def _(i):
        for r in range(rows):
            j = 0 if r == 0 else rows - 1 if r == 1 else r - 1
            zs[0, 0, r, i] = ab[0, j + 1, i + 1, pl.ds(0, 1)]
            zs[0, 1, r, i] = ab[0, j + 1, i + 1, pl.ds(depth - 1, 1)]

    @pl.loop(0, pieces)
    def _(n):
        each("start", sends, "down", lambda side: down(0, side, piece(n)))

    each("start", sends, "down", lambda side: down_inner(0, side))
    loads[1].wait()
    loads[2].wait()

    for m in range(pieces // 2):
        forward(0, m)

    level = lax.broadcasted_iota(jnp.int32, (depth, lanes), 0)

    def cell(now, later, j, i, r, final=False):
        x = ab[now, j + 1, i + 1]
        lower = jnp.where(level == 0, z[now, 0, r, i], pltpu.roll(x, 1, 0))
        upper = jnp.where(level == depth - 1, z[now, 1, r, i], pltpu.roll(x, depth - 1, 0))
        spread = (
            ab[now, j, i + 1] + ab[now, j + 2, i + 1]
            + ab[now, j + 1, i] + ab[now, j + 1, i + 2]
            + lower + upper - 6.0 * x
        )
        new = 2.0 * x - ab[later, j + 1, i + 1] + c[j, i] * spread
        if final:
            end[j, i] = new
            return
        ab[later, j + 1, i + 1] = new
        zs[later, 0, r, i] = new[:1]
        zs[later, 1, r, i] = new[depth - 1:]

    def inner(step, now, later, final=False):
        each("wait_recv", receives, "east", lambda side: east_inner(now, side))
        each("wait_recv", receives, "down", lambda side: down_inner(now, side))

        @pl.when(step >= 1)
        def _():
            each("wait_send", sends, "east", lambda side: east_inner(later, side))
            each("wait_send", sends, "down", lambda side: down_inner(later, side))

        @pl.loop(1, rows - 1)
        def _(j):
            @pl.loop(0, cols)
            def _(i):
                cell(now, later, j, i, j + 1, final)

        @pl.when(step < STEPS - 1)
        def _():
            each("start", sends, "east", lambda side: east_inner(later, side))
            each("start", sends, "down", lambda side: down_inner(later, side))

    def outer_edges(act, when, slot, n):
        for side in (0, 1):
            end = (0, pieces - 1)[side if when is sends else 1 - side]

            @pl.when(jnp.logical_and(when("east", side), n == end))
            def _():
                for k in (0, 1):
                    getattr(east(slot, side, k), act)()

    def outer_piece(step, now, later, turn, final=False):
        n = piece(turn)
        each("wait_recv", receives, "south", lambda side: south(now, side, n))
        each("wait_recv", receives, "down", lambda side: down(now, side, n))
        outer_edges("wait_recv", receives, now, n)

        @pl.when(step >= 1)
        def _():
            each("wait_send", sends, "south", lambda side: south(later, side, n))
            each("wait_send", sends, "down", lambda side: down(later, side, n))
            outer_edges("wait_send", sends, later, n)

        @pl.loop(0, wide)
        def _(w):
            i = n * wide + w
            cell(now, later, 0, i, 0, final)
            cell(now, later, rows - 1, i, 1, final)

        @pl.when(step < STEPS - 1)
        def _():
            send_south(step + 1, later, turn)
            each("start", sends, "down", lambda side: down(later, side, n))
            outer_edges("start", sends, later, n)

    @pl.loop(0, STEPS - 1)
    def _(step):
        now = lax.rem(step, 2)
        inner(step, now, 1 - now)

        @pl.loop(0, pieces)
        def _(n):
            outer_piece(step, now, 1 - now, n)
            if relays:
                @pl.when(jnp.logical_and(lax.rem(n, 2) == 1, n >= 3))
                def _():
                    forward(step + 1, n // 2 - 1)

        if relays:
            forward(step + 1, pieces // 2 - 1)

    last = STEPS - 1
    now, later = last % 2, 1 - last % 2
    inner(last, now, later, True)

    def carry(n):
        return remote(
            sbuf.at[pl.ds(n * wide, wide)], pin.at[pl.ds(n * wide, wide)],
            p_send.at[n], p_recv.at[n], "south", 1,
        )

    first = jnp.logical_not(below["south"])
    spot = place["south"]

    def total_copy(n, src, dst, way, kind, goal):
        part = pl.ds(n * wide, wide)
        return pltpu.make_async_remote_copy(
            src_ref=src.at[part], dst_ref=dst.at[part],
            send_sem=q_send.at[way, n], recv_sem=q_recv.at[kind, n],
            device_id={"south": goal}, device_id_type=MESH,
        )

    def beside(n):
        return total_copy(n, sbuf, pin, 0, 0, lax.rem(spot + 1, 4))

    def across(n):
        return total_copy(n, sbuf, pin, 1, 0, 2)

    def upward(n):
        return total_copy(n, sbuf, held, 1, 1, 3)

    def onward(n):
        return total_copy(n, held, held, 1, 1, 2)

    def middle_total(turn):
        n = piece(turn)

        @pl.when(spot == 2)
        def _():
            beside(n).wait_recv()

            @pl.loop(0, wide)
            def _(w):
                i = n * wide + w
                sbuf[i] = pin[i] + c[rows - 1, i]

            beside(n).start()

        @pl.when(spot == 3)
        def _():
            upward(n).wait_recv()
            onward(n).start()

    @pl.loop(0, pieces)
    def _(turn):
        n = piece(turn)
        outer_piece(last, now, later, turn, True)

        @pl.loop(0, wide)
        def _(w):
            i = n * wide + w
            sum_here = jnp.zeros((depth, lanes), jnp.float32)
            for j in range(rows):
                sum_here = sum_here + end[j, i]
                c[j, i] = sum_here * scale

        if square:
            @pl.when(spot < 2)
            def _():
                @pl.loop(0, wide)
                def _(w):
                    i = n * wide + w
                    sbuf[i] = c[rows - 1, i]

            @pl.when(spot == 0)
            def _():
                beside(n).start()
                across(n).start()

            @pl.when(spot == 1)
            def _():
                upward(n).start()

            @pl.when(turn >= 2)
            def _():
                middle_total(turn - 2)
        else:
            @pl.when(first)
            def _():
                @pl.loop(0, wide)
                def _(w):
                    i = n * wide + w
                    sbuf[i] = c[rows - 1, i]

                @pl.when(above["south"])
                def _():
                    carry(n).start()

    @pl.when(first)
    def _():
        @pl.loop(0, cols)
        def _(i):
            before[i] = blank

    if square:
        @pl.loop(pieces - 2, pieces)
        def _(turn):
            middle_total(turn)

        @pl.when(spot == 1)
        def _():
            @pl.loop(0, pieces)
            def _(turn):
                n = piece(turn)
                beside(n).wait_recv()

                @pl.loop(0, wide)
                def _(w):
                    i = n * wide + w
                    before[i] = pin[i]

        @pl.when(spot >= 2)
        def _():
            @pl.loop(0, pieces)
            def _(turn):
                n = piece(turn)

                @pl.when(spot == 2)
                def _():
                    upward(n).wait_recv()

                @pl.when(spot == 3)
                def _():
                    beside(n).wait_recv()

                @pl.loop(0, wide)
                def _(w):
                    i = n * wide + w
                    before[i] = pin[i] + held[i]
    else:
        @pl.when(below["south"])
        def _():
            @pl.loop(0, pieces)
            def _(turn):
                n = piece(turn)
                carry(n).wait_recv()

                @pl.loop(0, wide)
                def _(w):
                    i = n * wide + w
                    sbuf[i] = c[rows - 1, i] + pin[i]
                    before[i] = pin[i]

                @pl.when(above["south"])
                def _():
                    carry(n).start()

    if relays:
        @pl.when(is_relay)
        def _():
            for t in range(STEPS):
                for m in range(pieces // 2):
                    hop_out(t, m).wait_send()

    each("wait_send", sends, "east", lambda side: east_inner(now, side))
    each("wait_send", sends, "down", lambda side: down_inner(now, side))
    for k in (0, 1):
        each("wait_send", sends, "east", lambda side: east(now, side, k))

    @pl.loop(0, pieces)
    def _(n):
        each("wait_send", sends, "south", lambda side: south(now, side, n))
        each("wait_send", sends, "down", lambda side: down(now, side, n))

        if square:
            @pl.when(lax.rem(spot, 2) == 0)
            def _():
                beside(n).wait_send()

            @pl.when(spot != 2)
            def _():
                across(n).wait_send()
        else:
            @pl.when(above["south"])
            def _():
                carry(n).wait_send()


def writer(part, end, before, total_hbm, end_hbm, total, t_sem, e_sem):
    rows, cols = part.shape[:2]
    ends = [pltpu.make_async_copy(end.at[j], end_hbm.at[j], e_sem.at[j]) for j in range(rows)]
    totals = [
        pltpu.make_async_copy(total.at[j], total_hbm.at[j], t_sem.at[j]) for j in range(rows)
    ]
    for copy in ends:
        copy.start()
    for j in range(rows):
        @pl.loop(0, cols)
        def _(i):
            total[j, i] = part[j, i] + before[i]

        totals[j].start()
    for copy in ends + totals:
        copy.wait()


def shards(sizes, relays, field_now, earlier, speed_square):
    rows, cols, depth, lanes = field_now.shape
    pieces = min(PIECES, cols)
    relays = relays if pieces % 2 == 0 else {}
    edge = (2, 2, rows, cols, 1, lanes)
    dma = pltpu.SemaphoreType.DMA
    anywhere = pl.BlockSpec(memory_space=pltpu.HBM)
    inside = pl.BlockSpec(memory_space=pltpu.VMEM)
    part, end, before = pl.pallas_call(
        functools.partial(kernel, sizes, relays),
        out_shape=(
            pltpu.VMEM(field_now.shape, jnp.float32),
            pltpu.VMEM(field_now.shape, jnp.float32),
            pltpu.VMEM((cols, depth, lanes), jnp.float32),
        ),
        in_specs=[anywhere] * 3,
        out_specs=(inside,) * 3,
        scratch_shapes=[
            pltpu.VMEM((2, rows + 2, cols + 2, depth, lanes), jnp.float32),
            pltpu.VMEM(edge, jnp.float32),
            pltpu.VMEM(edge, jnp.float32),
            pltpu.VMEM((cols, depth, lanes), jnp.float32),
            pltpu.VMEM((cols, depth, lanes), jnp.float32),
            dma((2, 2, pieces)), dma((2, 2, pieces)),
            dma((2, 2, pieces)), dma((2, 2, pieces)),
            dma((2, 2, 2)), dma((2, 2, 2)),
            dma((2, 2)), dma((2, 2)), dma((2, 2)), dma((2, 2)),
            dma((pieces,)), dma((pieces,)), dma((5,)),
        ] + ([
            pltpu.VMEM((STEPS, pieces // 2, cols // pieces, depth, lanes), jnp.float32),
            dma((STEPS, pieces // 2)), dma((STEPS, pieces // 2)),
            pltpu.VMEM((cols, depth, lanes), jnp.float32),
            dma((2, pieces)), dma((2, pieces)),
        ] if relays else []),
        compiler_params=pltpu.CompilerParams(
            collective_id=0, has_side_effects=True, vmem_limit_bytes=VMEM_LIMIT
        ),
        name="wave",
    )(field_now, earlier, speed_square)
    return pl.pallas_call(
        writer,
        out_shape=(jax.ShapeDtypeStruct(field_now.shape, jnp.float32),) * 2,
        in_specs=[inside] * 3,
        out_specs=(anywhere,) * 2,
        scratch_shapes=[pltpu.VMEM(field_now.shape, jnp.float32), dma((rows,)), dma((rows,))],
        compiler_params=pltpu.CompilerParams(vmem_limit_bytes=WRITER_LIMIT),
        name="write",
    )(part, end, before)


def solution(mesh):
    placed = P("south", "east", "down", None)
    sizes = {axis: mesh.shape[axis] for axis in ("south", "east", "down")}
    relays = corner_relays(mesh)
    return jax.shard_map(
        functools.partial(shards, sizes, relays),
        mesh=mesh,
        in_specs=(placed,) * 3,
        out_specs=(placed,) * 2,
        check_vma=False,
    )
```

```python
import functools

import jax
import jax.numpy as jnp
import numpy as np
from jax import lax
from jax.experimental import pallas as pl
from jax.experimental.pallas import tpu as pltpu
from jax.sharding import PartitionSpec as P

STEPS = 4
PIECES = 8
VMEM_LIMIT = 42 * 1024 * 1024
WRITER_LIMIT = 12 * 1024 * 1024
VIA = 1
MESH = pl.DeviceIdType.MESH


def corner_relays(mesh):
    devices = mesh.devices
    if not hasattr(devices.flat[0], "coords"):
        return {}
    south = devices.shape[list(mesh.axis_names).index("south")]
    lines = np.moveaxis(devices, list(mesh.axis_names).index("south"), 0).reshape(south, -1)
    found = {}
    for side, pairs in ((0, [(p, p - 1) for p in range(1, south)]),
                        (1, [(p, p + 1) for p in range(south - 1)])):
        for p, q in pairs:
            choices = set()
            for line in range(lines.shape[1]):
                a, b = lines[p, line].coords, lines[q, line].coords
                differ = [d for d in range(3) if a[d] != b[d]]
                if len(differ) != 2 or any(abs(a[d] - b[d]) != 1 for d in differ):
                    choices.add(None)
                    continue
                corner = list(a)
                corner[differ[VIA]] = b[differ[VIA]]
                at = [r for r in range(south) if list(lines[r, line].coords) == corner]
                choices.add(at[0] if at else None)
            if len(choices) == 1 and None not in choices:
                found[p, side] = choices.pop()
    fits = all(abs(r - (p - 1 if side == 0 else p + 1)) == 1 for (p, side), r in found.items())
    if len(set(found.values())) != len(found) or not fits:
        return {}
    return found


def kernel(
    sizes, relays, u_hbm, e_hbm, c_hbm, c, end, before,
    ab, z, zs, pin, sbuf,
    s_send, s_recv, d_send, d_recv, e_send, e_recv,
    ei_send, ei_recv, di_send, di_recv, p_send, p_recv, load_sem, *hops,
):
    rows, cols, depth, lanes = u_hbm.shape
    pieces = min(PIECES, cols)
    wide = cols // pieces
    place = {axis: lax.axis_index(axis) for axis in sizes}
    below = {axis: place[axis] > 0 for axis in sizes}
    above = {axis: place[axis] < sizes[axis] - 1 for axis in sizes}
    scale = 1.0 / (rows * sizes["south"])

    odd = lax.rem(place["east"], 2) == 1

    def piece(n):
        return jnp.where(odd, n, pieces - 1 - n)

    def target(axis, side):
        step = sizes[axis] - 1 if side == 0 else 1
        return {axis: lax.rem(place[axis] + step, sizes[axis])}

    def sends(axis, side):
        return below[axis] if side == 0 else above[axis]

    def receives(axis, side):
        return above[axis] if side == 0 else below[axis]

    def remote(src, dst, send, recv, axis, side):
        return pltpu.make_async_remote_copy(
            src_ref=src, dst_ref=dst, send_sem=send, recv_sem=recv,
            device_id=target(axis, side), device_id_type=MESH,
        )

    def south(slot, side, n, first=False):
        here = (1, rows)[side]
        there = (rows + 1, 0)[side]
        src = (
            u_hbm.at[here - 1, pl.ds(n * wide, wide)]
            if first else ab.at[slot, here, pl.ds(n * wide + 1, wide)]
        )
        return remote(
            src, ab.at[slot, there, pl.ds(n * wide + 1, wide)],
            s_send.at[slot, side, n], s_recv.at[slot, side, n], "south", side,
        )

    def down(slot, side, n):
        part = (pl.ds(0, 2), pl.ds(n * wide, wide))
        return remote(
            zs.at[(slot, side) + part], z.at[(slot, 1 - side) + part],
            d_send.at[slot, side, n], d_recv.at[slot, side, n], "down", side,
        )

    def down_inner(slot, side):
        part = pl.ds(2, rows - 2)
        return remote(
            zs.at[slot, side, part], z.at[slot, 1 - side, part],
            di_send.at[slot, side], di_recv.at[slot, side], "down", side,
        )

    def east(slot, side, k, first=False):
        here = (1, cols)[side]
        there = (cols + 1, 0)[side]
        row = (1, rows)[k]
        src = u_hbm.at[row - 1, here - 1] if first else ab.at[slot, row, here]
        return remote(
            src, ab.at[slot, row, there],
            e_send.at[slot, side, k], e_recv.at[slot, side, k], "east", side,
        )

    def east_inner(slot, side, first=False):
        here = (1, cols)[side]
        there = (cols + 1, 0)[side]
        src = (
            u_hbm.at[pl.ds(1, rows - 2), here - 1]
            if first else ab.at[slot, pl.ds(2, rows - 2), here]
        )
        return remote(
            src, ab.at[slot, pl.ds(2, rows - 2), there],
            ei_send.at[slot, side], ei_recv.at[slot, side], "east", side,
        )

    square = False
    if relays:
        relay_buf, h_recv, h_send, held, q_send, q_recv = hops
    square = sizes["south"] == 4 and relays == {(2, 0): 0, (1, 1): 3}

    def by_place(table, other):
        value = jnp.int32(other)
        for p, entry in table.items():
            value = jnp.where(place["south"] == p, entry, value)
        return value

    relay_at = [
        by_place({p: r for (p, s), r in relays.items() if s == side}, -1) for side in (0, 1)
    ]
    served = by_place({r: p for (p, _), r in relays.items()}, -1)
    served_side = by_place({r: side for (_, side), r in relays.items()}, 0)
    is_relay = served >= 0

    def hop_in(t, slot, side, n, m, first=False):
        here = (1, rows)[side]
        src = (
            u_hbm.at[here - 1, pl.ds(n * wide, wide)]
            if first else ab.at[slot, here, pl.ds(n * wide + 1, wide)]
        )
        return pltpu.make_async_remote_copy(
            src_ref=src, dst_ref=relay_buf.at[t, m],
            send_sem=s_send.at[slot, side, n], recv_sem=h_recv.at[t, m],
            device_id={"south": jnp.maximum(relay_at[side], 0)}, device_id_type=MESH,
        )

    def hop_out(t, m):
        n = piece(2 * m + 1)
        slot = lax.rem(jnp.int32(t), 2)
        there = jnp.where(served_side == 0, rows + 1, 0)
        goal = served + 2 * served_side - 1
        return pltpu.make_async_remote_copy(
            src_ref=relay_buf.at[t, m],
            dst_ref=ab.at[slot, there, pl.ds(n * wide + 1, wide)],
            send_sem=h_send.at[t, m], recv_sem=s_recv.at[slot, served_side, n],
            device_id={"south": jnp.maximum(goal, 0)}, device_id_type=MESH,
        )

    def forward(t, m):
        if relays:
            @pl.when(is_relay)
            def _():
                hop_in(t, 0, 0, 0, m).wait_recv()
                hop_out(t, m).start()

    def send_south(t, slot, turn, first=False):
        n = piece(turn)
        for side in (0, 1):
            here = sends("south", side)
            if relays:
                bent = jnp.logical_and(relay_at[side] >= 0, lax.rem(turn, 2) == 1)

                @pl.when(jnp.logical_and(here, bent))
                def _():
                    hop_in(t, slot, side, n, turn // 2, first).start()

                here = jnp.logical_and(here, jnp.logical_not(bent))

            @pl.when(here)
            def _():
                south(slot, side, n, first).start()

    def each(act, when, axis, copy):
        for side in (0, 1):
            @pl.when(when(axis, side))
            def _():
                getattr(copy(side), act)()

    barrier = pltpu.get_barrier_semaphore()
    for axis in sizes:
        for side in (0, 1):
            @pl.when(sends(axis, side))
            def _():
                pl.semaphore_signal(
                    barrier, inc=1, device_id=target(axis, side), device_id_type=MESH
                )
    met = 0
    if relays:
        for side in (0, 1):
            @pl.when(relay_at[side] >= 0)
            def _():
                pl.semaphore_signal(
                    barrier, inc=1, device_id={"south": jnp.maximum(relay_at[side], 0)},
                    device_id_type=MESH,
                )

            met = met + (relay_at[side] >= 0).astype(jnp.int32)

        @pl.when(is_relay)
        def _():
            pl.semaphore_signal(
                barrier, inc=1, device_id={"south": jnp.maximum(served, 0)},
                device_id_type=MESH,
            )

        met = met + is_relay.astype(jnp.int32)
    for axis in sizes:
        met = met + below[axis].astype(jnp.int32) + above[axis].astype(jnp.int32)

    own = (pl.ds(1, rows), pl.ds(1, cols))
    loads = [
        pltpu.make_async_copy(u_hbm, ab.at[(0,) + own], load_sem.at[0]),
        pltpu.make_async_copy(e_hbm, ab.at[(1,) + own], load_sem.at[1]),
        pltpu.make_async_copy(c_hbm, c, load_sem.at[2]),
    ]
    loads[0].start()
    pl.semaphore_wait(barrier, met)

    @pl.loop(0, pieces)
    def _(n):
        send_south(0, 0, n, True)

    for k in (0, 1):
        each("start", sends, "east", lambda side: east(0, side, k, True))
    each("start", sends, "east", lambda side: east_inner(0, side, True))
    loads[1].start()
    loads[2].start()

    blank = jnp.zeros((depth, lanes), jnp.float32)
    for side, missing in ((0, below), (1, above)):
        @pl.when(jnp.logical_not(missing["south"]))
        def _():
            @pl.loop(0, cols)
            def _(i):
                for slot in (0, 1):
                    ab[slot, (0, rows + 1)[side], i + 1] = blank

        @pl.when(jnp.logical_not(missing["east"]))
        def _():
            @pl.loop(0, rows)
            def _(j):
                for slot in (0, 1):
                    ab[slot, j + 1, (0, cols + 1)[side]] = blank

        @pl.when(jnp.logical_not(missing["down"]))
        def _():
            @pl.loop(0, cols)
            def _(i):
                for slot in (0, 1):
                    for r in range(rows):
                        z[slot, side, r, i] = blank[:1]

    loads[0].wait()

    @pl.loop(0, cols)
    def _(i):
        for r in range(rows):
            j = 0 if r == 0 else rows - 1 if r == 1 else r - 1
            zs[0, 0, r, i] = ab[0, j + 1, i + 1, pl.ds(0, 1)]
            zs[0, 1, r, i] = ab[0, j + 1, i + 1, pl.ds(depth - 1, 1)]

    @pl.loop(0, pieces)
    def _(n):
        each("start", sends, "down", lambda side: down(0, side, piece(n)))

    each("start", sends, "down", lambda side: down_inner(0, side))
    loads[1].wait()
    loads[2].wait()

    for m in range(pieces // 2):
        forward(0, m)

    level = lax.broadcasted_iota(jnp.int32, (depth, lanes), 0)

    def cell(now, later, j, i, r, final=False):
        x = ab[now, j + 1, i + 1]
        lower = jnp.where(level == 0, z[now, 0, r, i], pltpu.roll(x, 1, 0))
        upper = jnp.where(level == depth - 1, z[now, 1, r, i], pltpu.roll(x, depth - 1, 0))
        spread = (
            ab[now, j, i + 1] + ab[now, j + 2, i + 1]
            + ab[now, j + 1, i] + ab[now, j + 1, i + 2]
            + lower + upper - 6.0 * x
        )
        new = 2.0 * x - ab[later, j + 1, i + 1] + c[j, i] * spread
        if final:
            end[j, i] = new
            return
        ab[later, j + 1, i + 1] = new
        zs[later, 0, r, i] = new[:1]
        zs[later, 1, r, i] = new[depth - 1:]

    def inner(step, now, later, final=False):
        each("wait_recv", receives, "east", lambda side: east_inner(now, side))
        each("wait_recv", receives, "down", lambda side: down_inner(now, side))

        @pl.when(step >= 1)
        def _():
            each("wait_send", sends, "east", lambda side: east_inner(later, side))
            each("wait_send", sends, "down", lambda side: down_inner(later, side))

        @pl.loop(1, rows - 1)
        def _(j):
            @pl.loop(0, cols)
            def _(i):
                cell(now, later, j, i, j + 1, final)

        @pl.when(step < STEPS - 1)
        def _():
            each("start", sends, "east", lambda side: east_inner(later, side))
            each("start", sends, "down", lambda side: down_inner(later, side))

    def outer_edges(act, when, slot, n):
        for side in (0, 1):
            end = (0, pieces - 1)[side if when is sends else 1 - side]

            @pl.when(jnp.logical_and(when("east", side), n == end))
            def _():
                for k in (0, 1):
                    getattr(east(slot, side, k), act)()

    def outer_piece(step, now, later, turn, final=False):
        n = piece(turn)
        each("wait_recv", receives, "south", lambda side: south(now, side, n))
        each("wait_recv", receives, "down", lambda side: down(now, side, n))
        outer_edges("wait_recv", receives, now, n)

        @pl.when(step >= 1)
        def _():
            each("wait_send", sends, "south", lambda side: south(later, side, n))
            each("wait_send", sends, "down", lambda side: down(later, side, n))
            outer_edges("wait_send", sends, later, n)

        @pl.loop(0, wide)
        def _(w):
            i = n * wide + w
            cell(now, later, 0, i, 0, final)
            cell(now, later, rows - 1, i, 1, final)

        @pl.when(step < STEPS - 1)
        def _():
            send_south(step + 1, later, turn)
            each("start", sends, "down", lambda side: down(later, side, n))
            outer_edges("start", sends, later, n)

    @pl.loop(0, STEPS - 1)
    def _(step):
        now = lax.rem(step, 2)
        inner(step, now, 1 - now)

        @pl.loop(0, pieces)
        def _(n):
            outer_piece(step, now, 1 - now, n)
            if relays:
                @pl.when(jnp.logical_and(lax.rem(n, 2) == 1, n >= 3))
                def _():
                    forward(step + 1, n // 2 - 1)

        if relays:
            forward(step + 1, pieces // 2 - 1)

    last = STEPS - 1
    now, later = last % 2, 1 - last % 2
    inner(last, now, later, True)

    def carry(n):
        return remote(
            sbuf.at[pl.ds(n * wide, wide)], pin.at[pl.ds(n * wide, wide)],
            p_send.at[n], p_recv.at[n], "south", 1,
        )

    first = jnp.logical_not(below["south"])
    spot = place["south"]

    def total_copy(n, src, dst, way, kind, goal):
        part = pl.ds(n * wide, wide)
        return pltpu.make_async_remote_copy(
            src_ref=src.at[part], dst_ref=dst.at[part],
            send_sem=q_send.at[way, n], recv_sem=q_recv.at[kind, n],
            device_id={"south": goal}, device_id_type=MESH,
        )

    def beside(n):
        return total_copy(n, sbuf, pin, 0, 0, lax.rem(spot + 1, 4))

    def across(n):
        return total_copy(n, sbuf, pin, 1, 0, 2)

    def upward(n):
        return total_copy(n, sbuf, held, 1, 1, 3)

    def direct(n):
        return total_copy(n, sbuf, held, 0, 1, 2)

    def onward(n):
        return total_copy(n, held, held, 1, 1, 2)

    def middle_total(turn):
        n = piece(turn)

        @pl.when(spot == 2)
        def _():
            beside(n).wait_recv()

            @pl.loop(0, wide)
            def _(w):
                i = n * wide + w
                sbuf[i] = pin[i] + c[rows - 1, i]

            beside(n).start()

        @pl.when(spot == 3)
        def _():
            upward(n).wait_recv()

            @pl.when(lax.rem(turn, 2) == 1)
            def _():
                onward(n).start()

    @pl.loop(0, pieces)
    def _(turn):
        n = piece(turn)
        outer_piece(last, now, later, turn, True)

        @pl.loop(0, wide)
        def _(w):
            i = n * wide + w
            sum_here = jnp.zeros((depth, lanes), jnp.float32)
            for j in range(rows):
                sum_here = sum_here + end[j, i]
                c[j, i] = sum_here * scale

        if square:
            @pl.when(spot < 2)
            def _():
                @pl.loop(0, wide)
                def _(w):
                    i = n * wide + w
                    sbuf[i] = c[rows - 1, i]

            @pl.when(spot == 0)
            def _():
                beside(n).start()
                across(n).start()

            @pl.when(spot == 1)
            def _():
                upward(n).start()

                @pl.when(lax.rem(turn, 2) == 0)
                def _():
                    direct(n).start()

            @pl.when(turn >= 2)
            def _():
                middle_total(turn - 2)
        else:
            @pl.when(first)
            def _():
                @pl.loop(0, wide)
                def _(w):
                    i = n * wide + w
                    sbuf[i] = c[rows - 1, i]

                @pl.when(above["south"])
                def _():
                    carry(n).start()

    @pl.when(first)
    def _():
        @pl.loop(0, cols)
        def _(i):
            before[i] = blank

    if square:
        @pl.loop(pieces - 2, pieces)
        def _(turn):
            middle_total(turn)

    if relays:
        @pl.when(is_relay)
        def _():
            for t in range(STEPS):
                for m in range(pieces // 2):
                    hop_out(t, m).wait_send()

    each("wait_send", sends, "east", lambda side: east_inner(now, side))
    each("wait_send", sends, "down", lambda side: down_inner(now, side))
    for k in (0, 1):
        each("wait_send", sends, "east", lambda side: east(now, side, k))

    @pl.loop(0, pieces)
    def _(n):
        each("wait_send", sends, "south", lambda side: south(now, side, n))
        each("wait_send", sends, "down", lambda side: down(now, side, n))

    if square:
        @pl.when(spot == 1)
        def _():
            @pl.loop(0, pieces)
            def _(turn):
                n = piece(turn)
                beside(n).wait_recv()

                @pl.loop(0, wide)
                def _(w):
                    i = n * wide + w
                    before[i] = pin[i]

        @pl.when(spot >= 2)
        def _():
            @pl.loop(0, pieces)
            def _(turn):
                n = piece(turn)

                @pl.when(spot == 2)
                def _():
                    upward(n).wait_recv()

                @pl.when(spot == 3)
                def _():
                    beside(n).wait_recv()

                @pl.loop(0, wide)
                def _(w):
                    i = n * wide + w
                    before[i] = pin[i] + held[i]
    else:
        @pl.when(below["south"])
        def _():
            @pl.loop(0, pieces)
            def _(turn):
                n = piece(turn)
                carry(n).wait_recv()

                @pl.loop(0, wide)
                def _(w):
                    i = n * wide + w
                    sbuf[i] = c[rows - 1, i] + pin[i]
                    before[i] = pin[i]

                @pl.when(above["south"])
                def _():
                    carry(n).start()

    @pl.loop(0, pieces)
    def _(turn):
        n = piece(turn)
        half = lax.rem(turn, 2)

        if square:
            @pl.when(jnp.logical_or(lax.rem(spot, 2) == 0, jnp.logical_and(spot == 1, half == 0)))
            def _():
                beside(n).wait_send()

            @pl.when(jnp.logical_or(spot < 2, jnp.logical_and(spot == 3, half == 1)))
            def _():
                across(n).wait_send()
        else:
            @pl.when(above["south"])
            def _():
                carry(n).wait_send()


def writer(part, end, before, total_hbm, end_hbm, total, t_sem, e_sem):
    rows, cols = part.shape[:2]
    ends = [pltpu.make_async_copy(end.at[j], end_hbm.at[j], e_sem.at[j]) for j in range(rows)]
    totals = [
        pltpu.make_async_copy(total.at[j], total_hbm.at[j], t_sem.at[j]) for j in range(rows)
    ]
    for copy in ends:
        copy.start()
    for j in range(rows):
        @pl.loop(0, cols)
        def _(i):
            total[j, i] = part[j, i] + before[i]

        totals[j].start()
    for copy in ends + totals:
        copy.wait()


def shards(sizes, relays, field_now, earlier, speed_square):
    rows, cols, depth, lanes = field_now.shape
    pieces = min(PIECES, cols)
    relays = relays if pieces % 2 == 0 else {}
    edge = (2, 2, rows, cols, 1, lanes)
    dma = pltpu.SemaphoreType.DMA
    anywhere = pl.BlockSpec(memory_space=pltpu.HBM)
    inside = pl.BlockSpec(memory_space=pltpu.VMEM)
    part, end, before = pl.pallas_call(
        functools.partial(kernel, sizes, relays),
        out_shape=(
            pltpu.VMEM(field_now.shape, jnp.float32),
            pltpu.VMEM(field_now.shape, jnp.float32),
            pltpu.VMEM((cols, depth, lanes), jnp.float32),
        ),
        in_specs=[anywhere] * 3,
        out_specs=(inside,) * 3,
        scratch_shapes=[
            pltpu.VMEM((2, rows + 2, cols + 2, depth, lanes), jnp.float32),
            pltpu.VMEM(edge, jnp.float32),
            pltpu.VMEM(edge, jnp.float32),
            pltpu.VMEM((cols, depth, lanes), jnp.float32),
            pltpu.VMEM((cols, depth, lanes), jnp.float32),
            dma((2, 2, pieces)), dma((2, 2, pieces)),
            dma((2, 2, pieces)), dma((2, 2, pieces)),
            dma((2, 2, 2)), dma((2, 2, 2)),
            dma((2, 2)), dma((2, 2)), dma((2, 2)), dma((2, 2)),
            dma((pieces,)), dma((pieces,)), dma((3,)),
        ] + ([
            pltpu.VMEM((STEPS, pieces // 2, cols // pieces, depth, lanes), jnp.float32),
            dma((STEPS, pieces // 2)), dma((STEPS, pieces // 2)),
            pltpu.VMEM((cols, depth, lanes), jnp.float32),
            dma((2, pieces)), dma((2, pieces)),
        ] if relays else []),
        compiler_params=pltpu.CompilerParams(
            collective_id=0, has_side_effects=True, vmem_limit_bytes=VMEM_LIMIT
        ),
        name="wave",
    )(field_now, earlier, speed_square)
    return pl.pallas_call(
        writer,
        out_shape=(jax.ShapeDtypeStruct(field_now.shape, jnp.float32),) * 2,
        in_specs=[inside] * 3,
        out_specs=(anywhere,) * 2,
        scratch_shapes=[pltpu.VMEM(field_now.shape, jnp.float32), dma((rows,)), dma((rows,))],
        compiler_params=pltpu.CompilerParams(vmem_limit_bytes=WRITER_LIMIT),
        name="write",
    )(part, end, before)


def solution(mesh):
    placed = P("south", "east", "down", None)
    sizes = {axis: mesh.shape[axis] for axis in ("south", "east", "down")}
    relays = corner_relays(mesh)
    return jax.shard_map(
        functools.partial(shards, sizes, relays),
        mesh=mesh,
        in_specs=(placed,) * 3,
        out_specs=(placed,) * 2,
        check_vma=False,
    )
```

```python
import functools

import jax
import jax.numpy as jnp
import numpy as np
from jax import lax
from jax.experimental import pallas as pl
from jax.experimental.pallas import tpu as pltpu
from jax.sharding import PartitionSpec as P

STEPS = 4
PIECES = 8
VMEM_LIMIT = 42 * 1024 * 1024
WRITER_LIMIT = 12 * 1024 * 1024
VIA = 1
MESH = pl.DeviceIdType.MESH


def corner_relays(mesh):
    devices = mesh.devices
    if not hasattr(devices.flat[0], "coords"):
        return {}
    south = devices.shape[list(mesh.axis_names).index("south")]
    lines = np.moveaxis(devices, list(mesh.axis_names).index("south"), 0).reshape(south, -1)
    found = {}
    for side, pairs in ((0, [(p, p - 1) for p in range(1, south)]),
                        (1, [(p, p + 1) for p in range(south - 1)])):
        for p, q in pairs:
            choices = set()
            for line in range(lines.shape[1]):
                a, b = lines[p, line].coords, lines[q, line].coords
                differ = [d for d in range(3) if a[d] != b[d]]
                if len(differ) != 2 or any(abs(a[d] - b[d]) != 1 for d in differ):
                    choices.add(None)
                    continue
                corner = list(a)
                corner[differ[VIA]] = b[differ[VIA]]
                at = [r for r in range(south) if list(lines[r, line].coords) == corner]
                choices.add(at[0] if at else None)
            if len(choices) == 1 and None not in choices:
                found[p, side] = choices.pop()
    fits = all(abs(r - (p - 1 if side == 0 else p + 1)) == 1 for (p, side), r in found.items())
    if len(set(found.values())) != len(found) or not fits:
        return {}
    return found


def kernel(
    sizes, relays, u_hbm, e_hbm, c_hbm, c, end, before,
    ab, z, zs, pin, sbuf,
    s_send, s_recv, d_send, d_recv, e_send, e_recv, ei_recv, di_recv, load_sem, *extra,
):
    rows, cols, depth, lanes = u_hbm.shape
    pieces = min(PIECES, cols)
    wide = cols // pieces
    groups = d_recv.shape[2]
    turns = pieces // groups
    square = is_square(sizes, relays)
    extra = list(extra)
    if relays:
        relay_buf, h_recv, h_send = extra[:3]
        del extra[:3]
    if square:
        held, q_send, q_recv = extra
    else:
        p_send, p_recv = extra
    place = {axis: lax.axis_index(axis) for axis in sizes}
    below = {axis: place[axis] > 0 for axis in sizes}
    above = {axis: place[axis] < sizes[axis] - 1 for axis in sizes}
    scale = 1.0 / (rows * sizes["south"])

    odd = lax.rem(place["east"], 2) == 1

    def piece(n):
        return jnp.where(odd, n, pieces - 1 - n)

    def target(axis, side):
        step = sizes[axis] - 1 if side == 0 else 1
        return {axis: lax.rem(place[axis] + step, sizes[axis])}

    def sends(axis, side):
        return below[axis] if side == 0 else above[axis]

    def receives(axis, side):
        return above[axis] if side == 0 else below[axis]

    def remote(src, dst, send, recv, axis, side):
        return pltpu.make_async_remote_copy(
            src_ref=src, dst_ref=dst, send_sem=send, recv_sem=recv,
            device_id=target(axis, side), device_id_type=MESH,
        )

    def south(slot, side, n, first=False):
        here = (1, rows)[side]
        there = (rows + 1, 0)[side]
        src = (
            u_hbm.at[here - 1, pl.ds(n * wide, wide)]
            if first else ab.at[slot, here, pl.ds(n * wide + 1, wide)]
        )
        return remote(
            src, ab.at[slot, there, pl.ds(n * wide + 1, wide)],
            s_send.at[slot, side], s_recv.at[slot, side, n], "south", side,
        )

    def south_sent(slot, side):
        row = ab.at[slot, (1, rows)[side], pl.ds(1, cols)]
        return remote(
            row, row, s_send.at[slot, side], s_recv.at[slot, side, 0], "south", side
        )

    def down(slot, side, group):
        start = jnp.where(odd, group, groups - 1 - group) * turns * wide
        part = (pl.ds(0, 2), pl.ds(start, turns * wide))
        return remote(
            zs.at[(slot, side) + part], z.at[(slot, 1 - side) + part],
            d_send.at[slot, side], d_recv.at[slot, side, group], "down", side,
        )

    def down_inner(slot, side):
        part = pl.ds(2, rows - 2)
        return remote(
            zs.at[slot, side, part], z.at[slot, 1 - side, part],
            d_send.at[slot, side], di_recv.at[slot, side], "down", side,
        )

    def down_sent(slot, side):
        return remote(
            zs.at[slot, side], z.at[slot, 1 - side],
            d_send.at[slot, side], di_recv.at[slot, side], "down", side,
        )

    def east(slot, side, k, first=False):
        here = (1, cols)[side]
        there = (cols + 1, 0)[side]
        row = (1, rows)[k]
        src = u_hbm.at[row - 1, here - 1] if first else ab.at[slot, row, here]
        return remote(
            src, ab.at[slot, row, there],
            e_send.at[slot, side], e_recv.at[slot, side], "east", side,
        )

    def east_both(slot, side):
        both = pl.ds(1, 2)
        return remote(
            ab.at[slot, both, (1, cols)[side]], ab.at[slot, both, (cols + 1, 0)[side]],
            e_send.at[slot, side], e_recv.at[slot, side], "east", side,
        )

    def east_inner(slot, side, first=False):
        here = (1, cols)[side]
        there = (cols + 1, 0)[side]
        src = (
            u_hbm.at[pl.ds(1, rows - 2), here - 1]
            if first else ab.at[slot, pl.ds(2, rows - 2), here]
        )
        return remote(
            src, ab.at[slot, pl.ds(2, rows - 2), there],
            e_send.at[slot, side], ei_recv.at[slot, side], "east", side,
        )

    def east_sent(slot, side):
        own = pl.ds(1, rows)
        return remote(
            ab.at[slot, own, (1, cols)[side]], ab.at[slot, own, (cols + 1, 0)[side]],
            e_send.at[slot, side], ei_recv.at[slot, side], "east", side,
        )

    def by_place(table, other):
        value = jnp.int32(other)
        for p, entry in table.items():
            value = jnp.where(place["south"] == p, entry, value)
        return value

    relay_at = [
        by_place({p: r for (p, s), r in relays.items() if s == side}, -1) for side in (0, 1)
    ]
    served = by_place({r: p for (p, _), r in relays.items()}, -1)
    served_side = by_place({r: side for (_, side), r in relays.items()}, 0)
    is_relay = served >= 0

    def hop_in(t, slot, side, n, m, first=False):
        here = (1, rows)[side]
        src = (
            u_hbm.at[here - 1, pl.ds(n * wide, wide)]
            if first else ab.at[slot, here, pl.ds(n * wide + 1, wide)]
        )
        return pltpu.make_async_remote_copy(
            src_ref=src, dst_ref=relay_buf.at[t, m],
            send_sem=s_send.at[slot, side], recv_sem=h_recv.at[lax.rem(jnp.int32(t), 2), m],
            device_id={"south": jnp.maximum(relay_at[side], 0)}, device_id_type=MESH,
        )

    def hop_out(t, m):
        n = piece(2 * m + 1)
        slot = lax.rem(jnp.int32(t), 2)
        there = jnp.where(served_side == 0, rows + 1, 0)
        goal = served + 2 * served_side - 1
        return pltpu.make_async_remote_copy(
            src_ref=relay_buf.at[t, m],
            dst_ref=ab.at[slot, there, pl.ds(n * wide + 1, wide)],
            send_sem=h_send.at[slot], recv_sem=s_recv.at[slot, served_side, n],
            device_id={"south": jnp.maximum(goal, 0)}, device_id_type=MESH,
        )

    def hops_sent(t):
        goal = served + 2 * served_side - 1
        return pltpu.make_async_remote_copy(
            src_ref=relay_buf.at[t], dst_ref=relay_buf.at[t],
            send_sem=h_send.at[lax.rem(jnp.int32(t), 2)], recv_sem=h_recv.at[0, 0],
            device_id={"south": jnp.maximum(goal, 0)}, device_id_type=MESH,
        )

    def forward(t, m):
        if relays:
            @pl.when(is_relay)
            def _():
                @pl.when(jnp.logical_and(t >= 2, m == 0))
                def _():
                    hops_sent(t - 2).wait_send()

                hop_in(t, 0, 0, 0, m).wait_recv()
                hop_out(t, m).start()

    def send_south(t, slot, turn, first=False):
        n = piece(turn)
        for side in (0, 1):
            here = sends("south", side)
            if relays:
                bent = jnp.logical_and(relay_at[side] >= 0, lax.rem(turn, 2) == 1)

                @pl.when(jnp.logical_and(here, bent))
                def _():
                    hop_in(t, slot, side, n, turn // 2, first).start()

                here = jnp.logical_and(here, jnp.logical_not(bent))

            @pl.when(here)
            def _():
                south(slot, side, n, first).start()

    def each(act, when, axis, copy):
        for side in (0, 1):
            @pl.when(when(axis, side))
            def _():
                getattr(copy(side), act)()

    barrier = pltpu.get_barrier_semaphore()
    for axis in sizes:
        for side in (0, 1):
            @pl.when(sends(axis, side))
            def _():
                pl.semaphore_signal(
                    barrier, inc=1, device_id=target(axis, side), device_id_type=MESH
                )
    met = 0
    if relays:
        for side in (0, 1):
            @pl.when(relay_at[side] >= 0)
            def _():
                pl.semaphore_signal(
                    barrier, inc=1, device_id={"south": jnp.maximum(relay_at[side], 0)},
                    device_id_type=MESH,
                )

            met = met + (relay_at[side] >= 0).astype(jnp.int32)

        @pl.when(is_relay)
        def _():
            pl.semaphore_signal(
                barrier, inc=1, device_id={"south": jnp.maximum(served, 0)},
                device_id_type=MESH,
            )

        met = met + is_relay.astype(jnp.int32)
    for axis in sizes:
        met = met + below[axis].astype(jnp.int32) + above[axis].astype(jnp.int32)

    own = (pl.ds(1, rows), pl.ds(1, cols))
    loads = [
        pltpu.make_async_copy(u_hbm, ab.at[(0,) + own], load_sem.at[0]),
        pltpu.make_async_copy(e_hbm, ab.at[(1,) + own], load_sem.at[1]),
        pltpu.make_async_copy(c_hbm, c, load_sem.at[2]),
    ]
    loads[0].start()
    pl.semaphore_wait(barrier, met)

    @pl.loop(0, pieces)
    def _(n):
        send_south(0, 0, n, True)

    for k in (0, 1):
        each("start", sends, "east", lambda side: east(0, side, k, True))
    each("start", sends, "east", lambda side: east_inner(0, side, True))
    loads[1].start()
    loads[2].start()

    blank = jnp.zeros((depth, lanes), jnp.float32)
    for side, missing in ((0, below), (1, above)):
        @pl.when(jnp.logical_not(missing["south"]))
        def _():
            @pl.loop(0, cols)
            def _(i):
                for slot in (0, 1):
                    ab[slot, (0, rows + 1)[side], i + 1] = blank

        @pl.when(jnp.logical_not(missing["east"]))
        def _():
            @pl.loop(0, rows)
            def _(j):
                for slot in (0, 1):
                    ab[slot, j + 1, (0, cols + 1)[side]] = blank

        @pl.when(jnp.logical_not(missing["down"]))
        def _():
            @pl.loop(0, cols)
            def _(i):
                for slot in (0, 1):
                    for r in range(rows):
                        z[slot, side, r, i] = blank[:1]

    loads[0].wait()

    @pl.loop(0, cols)
    def _(i):
        for r in range(rows):
            j = 0 if r == 0 else rows - 1 if r == 1 else r - 1
            zs[0, 0, r, i] = ab[0, j + 1, i + 1, pl.ds(0, 1)]
            zs[0, 1, r, i] = ab[0, j + 1, i + 1, pl.ds(depth - 1, 1)]

    for group in range(groups):
        each("start", sends, "down", lambda side: down(0, side, group))
    each("start", sends, "down", lambda side: down_inner(0, side))
    loads[1].wait()
    loads[2].wait()

    for m in range(pieces // 2):
        forward(0, m)

    level = lax.broadcasted_iota(jnp.int32, (depth, lanes), 0)

    def cell(now, later, j, i, r, final=False):
        x = ab[now, j + 1, i + 1]
        lower = jnp.where(level == 0, z[now, 0, r, i], pltpu.roll(x, 1, 0))
        upper = jnp.where(level == depth - 1, z[now, 1, r, i], pltpu.roll(x, depth - 1, 0))
        spread = (
            ab[now, j, i + 1] + ab[now, j + 2, i + 1]
            + ab[now, j + 1, i] + ab[now, j + 1, i + 2]
            + lower + upper - 6.0 * x
        )
        new = 2.0 * x - ab[later, j + 1, i + 1] + c[j, i] * spread
        if final:
            end[j, i] = new
            return
        ab[later, j + 1, i + 1] = new
        zs[later, 0, r, i] = new[:1]
        zs[later, 1, r, i] = new[depth - 1:]

    def inner(step, now, later, final=False):
        each("wait_recv", receives, "east", lambda side: east_inner(now, side))
        each("wait_recv", receives, "down", lambda side: down_inner(now, side))

        @pl.when(step >= 1)
        def _():
            each("wait_send", sends, "east", lambda side: east_sent(later, side))
            each("wait_send", sends, "down", lambda side: down_sent(later, side))
            each("wait_send", sends, "south", lambda side: south_sent(later, side))

        @pl.loop(1, rows - 1)
        def _(j):
            @pl.loop(0, cols)
            def _(i):
                cell(now, later, j, i, j + 1, final)

        @pl.when(step < STEPS - 1)
        def _():
            each("start", sends, "east", lambda side: east_inner(later, side))
            each("start", sends, "down", lambda side: down_inner(later, side))

    def edges_sent(slot, n):
        for side in (0, 1):
            @pl.when(jnp.logical_and(sends("east", side), n == (0, pieces - 1)[side]))
            def _():
                for k in (0, 1):
                    east(slot, side, k).start()

    def edges_received(slot, n):
        for side in (0, 1):
            @pl.when(jnp.logical_and(receives("east", side), n == (pieces - 1, 0)[side]))
            def _():
                east_both(slot, side).wait_recv()

    def outer_piece(step, now, later, turn, final=False):
        n = piece(turn)
        each("wait_recv", receives, "south", lambda side: south(now, side, n))

        @pl.when(lax.rem(turn, turns) == 0)
        def _():
            each("wait_recv", receives, "down", lambda side: down(now, side, turn // turns))

        edges_received(now, n)

        @pl.loop(0, wide)
        def _(w):
            i = n * wide + w
            cell(now, later, 0, i, 0, final)
            cell(now, later, rows - 1, i, 1, final)

        @pl.when(step < STEPS - 1)
        def _():
            send_south(step + 1, later, turn)

            @pl.when(lax.rem(turn, turns) == turns - 1)
            def _():
                each("start", sends, "down", lambda side: down(later, side, turn // turns))

            edges_sent(later, n)

    @pl.loop(0, STEPS - 1)
    def _(step):
        now = lax.rem(step, 2)
        inner(step, now, 1 - now)

        @pl.loop(0, pieces)
        def _(n):
            outer_piece(step, now, 1 - now, n)
            if relays:
                @pl.when(jnp.logical_and(lax.rem(n, 2) == 1, n >= 3))
                def _():
                    forward(step + 1, n // 2 - 1)

        if relays:
            forward(step + 1, pieces // 2 - 1)

    last = STEPS - 1
    now, later = last % 2, 1 - last % 2
    inner(last, now, later, True)

    def carry(n):
        return remote(
            sbuf.at[pl.ds(n * wide, wide)], pin.at[pl.ds(n * wide, wide)],
            p_send.at[0], p_recv.at[n], "south", 1,
        )

    first = jnp.logical_not(below["south"])
    spot = place["south"]

    def total_copy(n, src, dst, way, kind, goal):
        part = pl.ds(n * wide, wide)
        return pltpu.make_async_remote_copy(
            src_ref=src.at[part], dst_ref=dst.at[part],
            send_sem=q_send.at[way], recv_sem=q_recv.at[kind, n],
            device_id={"south": goal}, device_id_type=MESH,
        )

    def totals_sent(way):
        return pltpu.make_async_remote_copy(
            src_ref=sbuf, dst_ref=pin, send_sem=q_send.at[way], recv_sem=q_recv.at[0, 0],
            device_id={"south": lax.rem(spot + 1, 4)}, device_id_type=MESH,
        )

    def beside(n):
        return total_copy(n, sbuf, pin, 0, 0, lax.rem(spot + 1, 4))

    def across(n):
        return total_copy(n, sbuf, pin, 1, 0, 2)

    def upward(n):
        return total_copy(n, sbuf, held, 1, 1, 3)

    def onward(n):
        return total_copy(n, held, held, 1, 1, 2)

    def middle_total(turn):
        n = piece(turn)

        @pl.when(spot == 2)
        def _():
            beside(n).wait_recv()

            @pl.loop(0, wide)
            def _(w):
                i = n * wide + w
                sbuf[i] = pin[i] + c[rows - 1, i]

            beside(n).start()

        @pl.when(spot == 3)
        def _():
            upward(n).wait_recv()
            onward(n).start()

    @pl.loop(0, pieces)
    def _(turn):
        n = piece(turn)
        outer_piece(last, now, later, turn, True)

        @pl.loop(0, wide)
        def _(w):
            i = n * wide + w
            sum_here = jnp.zeros((depth, lanes), jnp.float32)
            for j in range(rows):
                sum_here = sum_here + end[j, i]
                c[j, i] = sum_here * scale

        if square:
            @pl.when(spot < 2)
            def _():
                @pl.loop(0, wide)
                def _(w):
                    i = n * wide + w
                    sbuf[i] = c[rows - 1, i]

            @pl.when(spot == 0)
            def _():
                beside(n).start()
                across(n).start()

            @pl.when(spot == 1)
            def _():
                upward(n).start()

            @pl.when(turn >= 2)
            def _():
                middle_total(turn - 2)
        else:
            @pl.when(first)
            def _():
                @pl.loop(0, wide)
                def _(w):
                    i = n * wide + w
                    sbuf[i] = c[rows - 1, i]

                @pl.when(above["south"])
                def _():
                    carry(n).start()

    @pl.when(first)
    def _():
        @pl.loop(0, cols)
        def _(i):
            before[i] = blank

    if square:
        @pl.loop(pieces - 2, pieces)
        def _(turn):
            middle_total(turn)

    if relays:
        @pl.when(is_relay)
        def _():
            for t in range(max(STEPS - 2, 0), STEPS):
                hops_sent(t).wait_send()

    each("wait_send", sends, "east", lambda side: east_sent(now, side))
    each("wait_send", sends, "down", lambda side: down_sent(now, side))
    each("wait_send", sends, "south", lambda side: south_sent(now, side))

    if square:
        @pl.when(spot == 1)
        def _():
            @pl.loop(0, pieces)
            def _(turn):
                n = piece(turn)
                beside(n).wait_recv()

                @pl.loop(0, wide)
                def _(w):
                    i = n * wide + w
                    before[i] = pin[i]

        @pl.when(spot >= 2)
        def _():
            @pl.loop(0, pieces)
            def _(turn):
                n = piece(turn)

                @pl.when(spot == 2)
                def _():
                    upward(n).wait_recv()

                @pl.when(spot == 3)
                def _():
                    beside(n).wait_recv()

                @pl.loop(0, wide)
                def _(w):
                    i = n * wide + w
                    before[i] = pin[i] + held[i]
    else:
        @pl.when(below["south"])
        def _():
            @pl.loop(0, pieces)
            def _(turn):
                n = piece(turn)
                carry(n).wait_recv()

                @pl.loop(0, wide)
                def _(w):
                    i = n * wide + w
                    sbuf[i] = c[rows - 1, i] + pin[i]
                    before[i] = pin[i]

                @pl.when(above["south"])
                def _():
                    carry(n).start()

    if square:
        @pl.when(lax.rem(spot, 2) == 0)
        def _():
            totals_sent(0).wait_send()

        @pl.when(spot != 2)
        def _():
            totals_sent(1).wait_send()
    else:
        @pl.when(above["south"])
        def _():
            remote(sbuf, pin, p_send.at[0], p_recv.at[0], "south", 1).wait_send()


def writer(part, end, before, total_hbm, end_hbm, total, sem):
    rows, cols = part.shape[:2]
    for j in range(rows):
        pltpu.make_async_copy(end.at[j], end_hbm.at[j], sem.at[0]).start()
    for j in range(rows):
        @pl.loop(0, cols)
        def _(i):
            total[j, i] = part[j, i] + before[i]

        pltpu.make_async_copy(total.at[j], total_hbm.at[j], sem.at[1]).start()
    pltpu.make_async_copy(end, end_hbm, sem.at[0]).wait()
    pltpu.make_async_copy(total, total_hbm, sem.at[1]).wait()


def is_square(sizes, relays):
    return sizes["south"] == 4 and relays == {(2, 0): 0, (1, 1): 3}


def shards(sizes, relays, field_now, earlier, speed_square):
    rows, cols, depth, lanes = field_now.shape
    pieces = min(PIECES, cols)
    relays = relays if pieces % 2 == 0 else {}
    groups = 2 if pieces % 2 == 0 else 1
    edge = (2, 2, rows, cols, 1, lanes)
    dma = pltpu.SemaphoreType.DMA
    anywhere = pl.BlockSpec(memory_space=pltpu.HBM)
    inside = pl.BlockSpec(memory_space=pltpu.VMEM)
    part, end, before = pl.pallas_call(
        functools.partial(kernel, sizes, relays),
        out_shape=(
            pltpu.VMEM(field_now.shape, jnp.float32),
            pltpu.VMEM(field_now.shape, jnp.float32),
            pltpu.VMEM((cols, depth, lanes), jnp.float32),
        ),
        in_specs=[anywhere] * 3,
        out_specs=(inside,) * 3,
        scratch_shapes=[
            pltpu.VMEM((2, rows + 2, cols + 2, depth, lanes), jnp.float32),
            pltpu.VMEM(edge, jnp.float32),
            pltpu.VMEM(edge, jnp.float32),
            pltpu.VMEM((cols, depth, lanes), jnp.float32),
            pltpu.VMEM((cols, depth, lanes), jnp.float32),
            dma((2, 2)), dma((2, 2, pieces)), dma((2, 2)), dma((2, 2, groups)),
            dma((2, 2)), dma((2, 2)), dma((2, 2)), dma((2, 2)), dma((3,)),
        ] + ([
            pltpu.VMEM((STEPS, pieces // 2, cols // pieces, depth, lanes), jnp.float32),
            dma((2, pieces // 2)), dma((2,)),
        ] if relays else []) + ([
            pltpu.VMEM((cols, depth, lanes), jnp.float32), dma((2,)), dma((2, pieces)),
        ] if is_square(sizes, relays) else [dma((1,)), dma((pieces,))]),
        compiler_params=pltpu.CompilerParams(
            collective_id=0, has_side_effects=True, vmem_limit_bytes=VMEM_LIMIT
        ),
        name="wave",
    )(field_now, earlier, speed_square)
    return pl.pallas_call(
        writer,
        out_shape=(jax.ShapeDtypeStruct(field_now.shape, jnp.float32),) * 2,
        in_specs=[inside] * 3,
        out_specs=(anywhere,) * 2,
        scratch_shapes=[pltpu.VMEM(field_now.shape, jnp.float32), dma((2,))],
        compiler_params=pltpu.CompilerParams(vmem_limit_bytes=WRITER_LIMIT),
        name="write",
    )(part, end, before)


def solution(mesh):
    placed = P("south", "east", "down", None)
    sizes = {axis: mesh.shape[axis] for axis in ("south", "east", "down")}
    relays = corner_relays(mesh)
    return jax.shard_map(
        functools.partial(shards, sizes, relays),
        mesh=mesh,
        in_specs=(placed,) * 3,
        out_specs=(placed,) * 2,
        check_vma=False,
    )
```

```python
import functools

import jax
import jax.numpy as jnp
import numpy as np
from jax import lax
from jax.experimental import pallas as pl
from jax.experimental.pallas import tpu as pltpu
from jax.sharding import PartitionSpec as P

STEPS = 4
PIECES = 4
VMEM_LIMIT = 42 * 1024 * 1024
WRITER_LIMIT = 12 * 1024 * 1024
VIA = 1
MESH = pl.DeviceIdType.MESH


def corner_relays(mesh):
    devices = mesh.devices
    if not hasattr(devices.flat[0], "coords"):
        return {}
    south = devices.shape[list(mesh.axis_names).index("south")]
    lines = np.moveaxis(devices, list(mesh.axis_names).index("south"), 0).reshape(south, -1)
    found = {}
    for side, pairs in ((0, [(p, p - 1) for p in range(1, south)]),
                        (1, [(p, p + 1) for p in range(south - 1)])):
        for p, q in pairs:
            choices = set()
            for line in range(lines.shape[1]):
                a, b = lines[p, line].coords, lines[q, line].coords
                differ = [d for d in range(3) if a[d] != b[d]]
                if len(differ) != 2 or any(abs(a[d] - b[d]) != 1 for d in differ):
                    choices.add(None)
                    continue
                corner = list(a)
                corner[differ[VIA]] = b[differ[VIA]]
                at = [r for r in range(south) if list(lines[r, line].coords) == corner]
                choices.add(at[0] if at else None)
            if len(choices) == 1 and None not in choices:
                found[p, side] = choices.pop()
    fits = all(abs(r - (p - 1 if side == 0 else p + 1)) == 1 for (p, side), r in found.items())
    if len(set(found.values())) != len(found) or not fits:
        return {}
    return found


def kernel(
    sizes, relays, u_hbm, e_hbm, c_hbm, c, end, before,
    ab, z, zs, pin, sbuf,
    s_send, s_recv, d_send, d_recv, e_send, e_recv, ei_recv, di_recv, load_sem, *extra,
):
    rows, cols, depth, lanes = u_hbm.shape
    pieces = min(PIECES, cols)
    wide = cols // pieces
    groups = d_recv.shape[2]
    turns = pieces // groups
    square = is_square(sizes, relays)
    extra = list(extra)
    if relays:
        relay_buf, h_recv, h_send = extra[:3]
        del extra[:3]
    if square:
        held, q_send, q_recv = extra
    else:
        p_send, p_recv = extra
    place = {axis: lax.axis_index(axis) for axis in sizes}
    below = {axis: place[axis] > 0 for axis in sizes}
    above = {axis: place[axis] < sizes[axis] - 1 for axis in sizes}
    scale = 1.0 / (rows * sizes["south"])

    odd = lax.rem(place["east"], 2) == 1

    def piece(n):
        return jnp.where(odd, n, pieces - 1 - n)

    def target(axis, side):
        step = sizes[axis] - 1 if side == 0 else 1
        return {axis: lax.rem(place[axis] + step, sizes[axis])}

    def sends(axis, side):
        return below[axis] if side == 0 else above[axis]

    def receives(axis, side):
        return above[axis] if side == 0 else below[axis]

    def remote(src, dst, send, recv, axis, side):
        return pltpu.make_async_remote_copy(
            src_ref=src, dst_ref=dst, send_sem=send, recv_sem=recv,
            device_id=target(axis, side), device_id_type=MESH,
        )

    def south(slot, side, n, first=False):
        here = (1, rows)[side]
        there = (rows + 1, 0)[side]
        src = (
            u_hbm.at[here - 1, pl.ds(n * wide, wide)]
            if first else ab.at[slot, here, pl.ds(n * wide + 1, wide)]
        )
        return remote(
            src, ab.at[slot, there, pl.ds(n * wide + 1, wide)],
            s_send.at[slot, side], s_recv.at[slot, side, n], "south", side,
        )

    def south_sent(slot, side):
        row = ab.at[slot, (1, rows)[side], pl.ds(1, cols)]
        return remote(
            row, row, s_send.at[slot, side], s_recv.at[slot, side, 0], "south", side
        )

    def down(slot, side, group):
        start = jnp.where(odd, group, groups - 1 - group) * turns * wide
        part = (pl.ds(0, 2), pl.ds(start, turns * wide))
        return remote(
            zs.at[(slot, side) + part], z.at[(slot, 1 - side) + part],
            d_send.at[slot, side], d_recv.at[slot, side, group], "down", side,
        )

    def down_inner(slot, side):
        part = pl.ds(2, rows - 2)
        return remote(
            zs.at[slot, side, part], z.at[slot, 1 - side, part],
            d_send.at[slot, side], di_recv.at[slot, side], "down", side,
        )

    def down_sent(slot, side):
        return remote(
            zs.at[slot, side], z.at[slot, 1 - side],
            d_send.at[slot, side], di_recv.at[slot, side], "down", side,
        )

    def east(slot, side, k, first=False):
        here = (1, cols)[side]
        there = (cols + 1, 0)[side]
        row = (1, rows)[k]
        src = u_hbm.at[row - 1, here - 1] if first else ab.at[slot, row, here]
        return remote(
            src, ab.at[slot, row, there],
            e_send.at[slot, side], e_recv.at[slot, side], "east", side,
        )

    def east_both(slot, side):
        both = pl.ds(1, 2)
        return remote(
            ab.at[slot, both, (1, cols)[side]], ab.at[slot, both, (cols + 1, 0)[side]],
            e_send.at[slot, side], e_recv.at[slot, side], "east", side,
        )

    def east_inner(slot, side, first=False):
        here = (1, cols)[side]
        there = (cols + 1, 0)[side]
        src = (
            u_hbm.at[pl.ds(1, rows - 2), here - 1]
            if first else ab.at[slot, pl.ds(2, rows - 2), here]
        )
        return remote(
            src, ab.at[slot, pl.ds(2, rows - 2), there],
            e_send.at[slot, side], ei_recv.at[slot, side], "east", side,
        )

    def east_sent(slot, side):
        own = pl.ds(1, rows)
        return remote(
            ab.at[slot, own, (1, cols)[side]], ab.at[slot, own, (cols + 1, 0)[side]],
            e_send.at[slot, side], ei_recv.at[slot, side], "east", side,
        )

    def by_place(table, other):
        value = jnp.int32(other)
        for p, entry in table.items():
            value = jnp.where(place["south"] == p, entry, value)
        return value

    relay_at = [
        by_place({p: r for (p, s), r in relays.items() if s == side}, -1) for side in (0, 1)
    ]
    served = by_place({r: p for (p, _), r in relays.items()}, -1)
    served_side = by_place({r: side for (_, side), r in relays.items()}, 0)
    is_relay = served >= 0

    def hop_in(t, slot, side, n, m, first=False):
        here = (1, rows)[side]
        src = (
            u_hbm.at[here - 1, pl.ds(n * wide, wide)]
            if first else ab.at[slot, here, pl.ds(n * wide + 1, wide)]
        )
        return pltpu.make_async_remote_copy(
            src_ref=src, dst_ref=relay_buf.at[t, m],
            send_sem=s_send.at[slot, side], recv_sem=h_recv.at[lax.rem(jnp.int32(t), 2), m],
            device_id={"south": jnp.maximum(relay_at[side], 0)}, device_id_type=MESH,
        )

    def hop_out(t, m):
        n = piece(2 * m + 1)
        slot = lax.rem(jnp.int32(t), 2)
        there = jnp.where(served_side == 0, rows + 1, 0)
        goal = served + 2 * served_side - 1
        return pltpu.make_async_remote_copy(
            src_ref=relay_buf.at[t, m],
            dst_ref=ab.at[slot, there, pl.ds(n * wide + 1, wide)],
            send_sem=h_send.at[slot], recv_sem=s_recv.at[slot, served_side, n],
            device_id={"south": jnp.maximum(goal, 0)}, device_id_type=MESH,
        )

    def hops_sent(t):
        goal = served + 2 * served_side - 1
        return pltpu.make_async_remote_copy(
            src_ref=relay_buf.at[t], dst_ref=relay_buf.at[t],
            send_sem=h_send.at[lax.rem(jnp.int32(t), 2)], recv_sem=h_recv.at[0, 0],
            device_id={"south": jnp.maximum(goal, 0)}, device_id_type=MESH,
        )

    def forward(t, m):
        if relays:
            @pl.when(is_relay)
            def _():
                @pl.when(jnp.logical_and(t >= 2, m == 0))
                def _():
                    hops_sent(t - 2).wait_send()

                hop_in(t, 0, 0, 0, m).wait_recv()
                hop_out(t, m).start()

    def send_south(t, slot, turn, first=False):
        n = piece(turn)
        for side in (0, 1):
            here = sends("south", side)
            if relays:
                bent = jnp.logical_and(relay_at[side] >= 0, lax.rem(turn, 2) == 1)

                @pl.when(jnp.logical_and(here, bent))
                def _():
                    hop_in(t, slot, side, n, turn // 2, first).start()

                here = jnp.logical_and(here, jnp.logical_not(bent))

            @pl.when(here)
            def _():
                south(slot, side, n, first).start()

    def each(act, when, axis, copy):
        for side in (0, 1):
            @pl.when(when(axis, side))
            def _():
                getattr(copy(side), act)()

    barrier = pltpu.get_barrier_semaphore()
    for axis in sizes:
        for side in (0, 1):
            @pl.when(sends(axis, side))
            def _():
                pl.semaphore_signal(
                    barrier, inc=1, device_id=target(axis, side), device_id_type=MESH
                )
    met = 0
    if relays:
        for side in (0, 1):
            @pl.when(relay_at[side] >= 0)
            def _():
                pl.semaphore_signal(
                    barrier, inc=1, device_id={"south": jnp.maximum(relay_at[side], 0)},
                    device_id_type=MESH,
                )

            met = met + (relay_at[side] >= 0).astype(jnp.int32)

        @pl.when(is_relay)
        def _():
            pl.semaphore_signal(
                barrier, inc=1, device_id={"south": jnp.maximum(served, 0)},
                device_id_type=MESH,
            )

        met = met + is_relay.astype(jnp.int32)
    for axis in sizes:
        met = met + below[axis].astype(jnp.int32) + above[axis].astype(jnp.int32)

    own = (pl.ds(1, rows), pl.ds(1, cols))
    loads = [
        pltpu.make_async_copy(u_hbm, ab.at[(0,) + own], load_sem.at[0]),
        pltpu.make_async_copy(e_hbm, ab.at[(1,) + own], load_sem.at[1]),
        pltpu.make_async_copy(c_hbm, c, load_sem.at[2]),
    ]
    loads[0].start()
    pl.semaphore_wait(barrier, met)

    @pl.loop(0, pieces)
    def _(n):
        send_south(0, 0, n, True)

    for k in (0, 1):
        each("start", sends, "east", lambda side: east(0, side, k, True))
    each("start", sends, "east", lambda side: east_inner(0, side, True))
    loads[1].start()
    loads[2].start()

    blank = jnp.zeros((depth, lanes), jnp.float32)
    for side, missing in ((0, below), (1, above)):
        @pl.when(jnp.logical_not(missing["south"]))
        def _():
            @pl.loop(0, cols)
            def _(i):
                for slot in (0, 1):
                    ab[slot, (0, rows + 1)[side], i + 1] = blank

        @pl.when(jnp.logical_not(missing["east"]))
        def _():
            @pl.loop(0, rows)
            def _(j):
                for slot in (0, 1):
                    ab[slot, j + 1, (0, cols + 1)[side]] = blank

        @pl.when(jnp.logical_not(missing["down"]))
        def _():
            @pl.loop(0, cols)
            def _(i):
                for slot in (0, 1):
                    for r in range(rows):
                        z[slot, side, r, i] = blank[:1]

    loads[0].wait()

    @pl.loop(0, cols)
    def _(i):
        for r in range(rows):
            j = 0 if r == 0 else rows - 1 if r == 1 else r - 1
            zs[0, 0, r, i] = ab[0, j + 1, i + 1, pl.ds(0, 1)]
            zs[0, 1, r, i] = ab[0, j + 1, i + 1, pl.ds(depth - 1, 1)]

    for group in range(groups):
        each("start", sends, "down", lambda side: down(0, side, group))
    each("start", sends, "down", lambda side: down_inner(0, side))
    loads[1].wait()
    loads[2].wait()

    for m in range(pieces // 2):
        forward(0, m)

    level = lax.broadcasted_iota(jnp.int32, (depth, lanes), 0)

    def cell(now, later, j, i, r, final=False):
        x = ab[now, j + 1, i + 1]
        lower = jnp.where(level == 0, z[now, 0, r, i], pltpu.roll(x, 1, 0))
        upper = jnp.where(level == depth - 1, z[now, 1, r, i], pltpu.roll(x, depth - 1, 0))
        spread = (
            ab[now, j, i + 1] + ab[now, j + 2, i + 1]
            + ab[now, j + 1, i] + ab[now, j + 1, i + 2]
            + lower + upper - 6.0 * x
        )
        new = 2.0 * x - ab[later, j + 1, i + 1] + c[j, i] * spread
        if final:
            end[j, i] = new
            return
        ab[later, j + 1, i + 1] = new
        zs[later, 0, r, i] = new[:1]
        zs[later, 1, r, i] = new[depth - 1:]

    def inner(step, now, later, final=False):
        each("wait_recv", receives, "east", lambda side: east_inner(now, side))
        each("wait_recv", receives, "down", lambda side: down_inner(now, side))

        @pl.when(step >= 1)
        def _():
            each("wait_send", sends, "east", lambda side: east_sent(later, side))
            each("wait_send", sends, "down", lambda side: down_sent(later, side))
            each("wait_send", sends, "south", lambda side: south_sent(later, side))

        @pl.loop(1, rows - 1)
        def _(j):
            @pl.loop(0, cols)
            def _(i):
                cell(now, later, j, i, j + 1, final)

        @pl.when(step < STEPS - 1)
        def _():
            each("start", sends, "east", lambda side: east_inner(later, side))
            each("start", sends, "down", lambda side: down_inner(later, side))

    def edges_sent(slot, n):
        for side in (0, 1):
            @pl.when(jnp.logical_and(sends("east", side), n == (0, pieces - 1)[side]))
            def _():
                for k in (0, 1):
                    east(slot, side, k).start()

    def edges_received(slot, n):
        for side in (0, 1):
            @pl.when(jnp.logical_and(receives("east", side), n == (pieces - 1, 0)[side]))
            def _():
                east_both(slot, side).wait_recv()

    def outer_piece(step, now, later, turn, final=False):
        n = piece(turn)
        each("wait_recv", receives, "south", lambda side: south(now, side, n))

        @pl.when(lax.rem(turn, turns) == 0)
        def _():
            each("wait_recv", receives, "down", lambda side: down(now, side, turn // turns))

        edges_received(now, n)

        @pl.loop(0, wide)
        def _(w):
            i = n * wide + w
            cell(now, later, 0, i, 0, final)
            cell(now, later, rows - 1, i, 1, final)

        @pl.when(step < STEPS - 1)
        def _():
            send_south(step + 1, later, turn)

            @pl.when(lax.rem(turn, turns) == turns - 1)
            def _():
                each("start", sends, "down", lambda side: down(later, side, turn // turns))

            edges_sent(later, n)

    @pl.loop(0, STEPS - 1)
    def _(step):
        now = lax.rem(step, 2)
        inner(step, now, 1 - now)

        @pl.loop(0, pieces)
        def _(n):
            outer_piece(step, now, 1 - now, n)
            if relays:
                @pl.when(jnp.logical_and(lax.rem(n, 2) == 1, n >= 3))
                def _():
                    forward(step + 1, n // 2 - 1)

        if relays:
            forward(step + 1, pieces // 2 - 1)

    last = STEPS - 1
    now, later = last % 2, 1 - last % 2
    inner(last, now, later, True)

    def carry(n):
        return remote(
            sbuf.at[pl.ds(n * wide, wide)], pin.at[pl.ds(n * wide, wide)],
            p_send.at[0], p_recv.at[n], "south", 1,
        )

    first = jnp.logical_not(below["south"])
    spot = place["south"]

    def total_copy(n, src, dst, way, kind, goal):
        part = pl.ds(n * wide, wide)
        return pltpu.make_async_remote_copy(
            src_ref=src.at[part], dst_ref=dst.at[part],
            send_sem=q_send.at[way], recv_sem=q_recv.at[kind, n],
            device_id={"south": goal}, device_id_type=MESH,
        )

    early = pieces // 4

    def totals_sent(way, count=pieces):
        part = pl.ds(0, count * wide)
        return pltpu.make_async_remote_copy(
            src_ref=sbuf.at[part], dst_ref=pin.at[part],
            send_sem=q_send.at[way], recv_sem=q_recv.at[0, 0],
            device_id={"south": lax.rem(spot + 1, 4)}, device_id_type=MESH,
        )

    def beside(n):
        return total_copy(n, sbuf, pin, 0, 0, lax.rem(spot + 1, 4))

    def across(n):
        return total_copy(n, sbuf, pin, 1, 0, 2)

    def upward(n):
        return total_copy(n, sbuf, held, 1, 1, 3)

    def direct(n):
        return total_copy(n, sbuf, held, 0, 1, 2)

    def onward(n):
        return total_copy(n, held, held, 1, 1, 2)

    def middle_total(turn):
        n = piece(turn)

        @pl.when(spot == 2)
        def _():
            beside(n).wait_recv()

            @pl.loop(0, wide)
            def _(w):
                i = n * wide + w
                sbuf[i] = pin[i] + c[rows - 1, i]

            beside(n).start()

        @pl.when(spot == 3)
        def _():
            upward(n).wait_recv()

            @pl.when(turn >= early)
            def _():
                onward(n).start()

    @pl.loop(0, pieces)
    def _(turn):
        n = piece(turn)
        outer_piece(last, now, later, turn, True)

        @pl.loop(0, wide)
        def _(w):
            i = n * wide + w
            sum_here = jnp.zeros((depth, lanes), jnp.float32)
            for j in range(rows):
                sum_here = sum_here + end[j, i]
                c[j, i] = sum_here * scale

        if square:
            @pl.when(spot < 2)
            def _():
                @pl.loop(0, wide)
                def _(w):
                    i = n * wide + w
                    sbuf[i] = c[rows - 1, i]

            @pl.when(spot == 0)
            def _():
                beside(n).start()
                across(n).start()

            @pl.when(spot == 1)
            def _():
                upward(n).start()

                @pl.when(turn < early)
                def _():
                    direct(n).start()

            @pl.when(turn >= 2)
            def _():
                middle_total(turn - 2)
        else:
            @pl.when(first)
            def _():
                @pl.loop(0, wide)
                def _(w):
                    i = n * wide + w
                    sbuf[i] = c[rows - 1, i]

                @pl.when(above["south"])
                def _():
                    carry(n).start()

    @pl.when(first)
    def _():
        @pl.loop(0, cols)
        def _(i):
            before[i] = blank

    if square:
        @pl.loop(pieces - 2, pieces)
        def _(turn):
            middle_total(turn)

    if relays:
        @pl.when(is_relay)
        def _():
            for t in range(max(STEPS - 2, 0), STEPS):
                hops_sent(t).wait_send()

    each("wait_send", sends, "east", lambda side: east_sent(now, side))
    each("wait_send", sends, "down", lambda side: down_sent(now, side))
    each("wait_send", sends, "south", lambda side: south_sent(now, side))

    if square:
        @pl.when(spot == 1)
        def _():
            @pl.loop(0, pieces)
            def _(turn):
                n = piece(turn)
                beside(n).wait_recv()

                @pl.loop(0, wide)
                def _(w):
                    i = n * wide + w
                    before[i] = pin[i]

        @pl.when(spot >= 2)
        def _():
            @pl.loop(0, pieces)
            def _(turn):
                n = piece(turn)

                @pl.when(spot == 2)
                def _():
                    upward(n).wait_recv()

                @pl.when(spot == 3)
                def _():
                    beside(n).wait_recv()

                @pl.loop(0, wide)
                def _(w):
                    i = n * wide + w
                    before[i] = pin[i] + held[i]
    else:
        @pl.when(below["south"])
        def _():
            @pl.loop(0, pieces)
            def _(turn):
                n = piece(turn)
                carry(n).wait_recv()

                @pl.loop(0, wide)
                def _(w):
                    i = n * wide + w
                    sbuf[i] = c[rows - 1, i] + pin[i]
                    before[i] = pin[i]

                @pl.when(above["south"])
                def _():
                    carry(n).start()

    if square:
        @pl.when(lax.rem(spot, 2) == 0)
        def _():
            totals_sent(0).wait_send()

        @pl.when(spot < 2)
        def _():
            totals_sent(1).wait_send()

        if early:
            @pl.when(spot == 1)
            def _():
                totals_sent(0, early).wait_send()

        @pl.when(spot == 3)
        def _():
            totals_sent(1, pieces - early).wait_send()
    else:
        @pl.when(above["south"])
        def _():
            remote(sbuf, pin, p_send.at[0], p_recv.at[0], "south", 1).wait_send()


def writer(part, end, before, total_hbm, end_hbm, total, sem):
    rows, cols = part.shape[:2]
    for j in range(rows):
        pltpu.make_async_copy(end.at[j], end_hbm.at[j], sem.at[0]).start()
    for j in range(rows):
        @pl.loop(0, cols)
        def _(i):
            total[j, i] = part[j, i] + before[i]

        pltpu.make_async_copy(total.at[j], total_hbm.at[j], sem.at[1]).start()
    pltpu.make_async_copy(end, end_hbm, sem.at[0]).wait()
    pltpu.make_async_copy(total, total_hbm, sem.at[1]).wait()


def is_square(sizes, relays):
    return sizes["south"] == 4 and relays == {(2, 0): 0, (1, 1): 3}


def shards(sizes, relays, field_now, earlier, speed_square):
    rows, cols, depth, lanes = field_now.shape
    pieces = min(PIECES, cols)
    relays = relays if pieces % 2 == 0 else {}
    groups = 2 if pieces % 2 == 0 else 1
    edge = (2, 2, rows, cols, 1, lanes)
    dma = pltpu.SemaphoreType.DMA
    anywhere = pl.BlockSpec(memory_space=pltpu.HBM)
    inside = pl.BlockSpec(memory_space=pltpu.VMEM)
    part, end, before = pl.pallas_call(
        functools.partial(kernel, sizes, relays),
        out_shape=(
            pltpu.VMEM(field_now.shape, jnp.float32),
            pltpu.VMEM(field_now.shape, jnp.float32),
            pltpu.VMEM((cols, depth, lanes), jnp.float32),
        ),
        in_specs=[anywhere] * 3,
        out_specs=(inside,) * 3,
        scratch_shapes=[
            pltpu.VMEM((2, rows + 2, cols + 2, depth, lanes), jnp.float32),
            pltpu.VMEM(edge, jnp.float32),
            pltpu.VMEM(edge, jnp.float32),
            pltpu.VMEM((cols, depth, lanes), jnp.float32),
            pltpu.VMEM((cols, depth, lanes), jnp.float32),
            dma((2, 2)), dma((2, 2, pieces)), dma((2, 2)), dma((2, 2, groups)),
            dma((2, 2)), dma((2, 2)), dma((2, 2)), dma((2, 2)), dma((3,)),
        ] + ([
            pltpu.VMEM((STEPS, pieces // 2, cols // pieces, depth, lanes), jnp.float32),
            dma((2, pieces // 2)), dma((2,)),
        ] if relays else []) + ([
            pltpu.VMEM((cols, depth, lanes), jnp.float32), dma((2,)), dma((2, pieces)),
        ] if is_square(sizes, relays) else [dma((1,)), dma((pieces,))]),
        compiler_params=pltpu.CompilerParams(
            collective_id=0, has_side_effects=True, vmem_limit_bytes=VMEM_LIMIT
        ),
        name="wave",
    )(field_now, earlier, speed_square)
    return pl.pallas_call(
        writer,
        out_shape=(jax.ShapeDtypeStruct(field_now.shape, jnp.float32),) * 2,
        in_specs=[inside] * 3,
        out_specs=(anywhere,) * 2,
        scratch_shapes=[pltpu.VMEM(field_now.shape, jnp.float32), dma((2,))],
        compiler_params=pltpu.CompilerParams(vmem_limit_bytes=WRITER_LIMIT),
        name="write",
    )(part, end, before)


def solution(mesh):
    placed = P("south", "east", "down", None)
    sizes = {axis: mesh.shape[axis] for axis in ("south", "east", "down")}
    relays = corner_relays(mesh)
    return jax.shard_map(
        functools.partial(shards, sizes, relays),
        mesh=mesh,
        in_specs=(placed,) * 3,
        out_specs=(placed,) * 2,
        check_vma=False,
    )
```

```python
import functools

import jax
import jax.numpy as jnp
import numpy as np
from jax import lax
from jax.experimental import pallas as pl
from jax.experimental.pallas import tpu as pltpu
from jax.sharding import PartitionSpec as P

STEPS = 4
PIECES = 4
VMEM_LIMIT = 42 * 1024 * 1024
WRITER_LIMIT = 12 * 1024 * 1024
VIA = 1
MESH = pl.DeviceIdType.MESH


def corner_relays(mesh):
    devices = mesh.devices
    if not hasattr(devices.flat[0], "coords"):
        return {}
    south = devices.shape[list(mesh.axis_names).index("south")]
    lines = np.moveaxis(devices, list(mesh.axis_names).index("south"), 0).reshape(south, -1)
    found = {}
    for side, pairs in ((0, [(p, p - 1) for p in range(1, south)]),
                        (1, [(p, p + 1) for p in range(south - 1)])):
        for p, q in pairs:
            choices = set()
            for line in range(lines.shape[1]):
                a, b = lines[p, line].coords, lines[q, line].coords
                differ = [d for d in range(3) if a[d] != b[d]]
                if len(differ) != 2 or any(abs(a[d] - b[d]) != 1 for d in differ):
                    choices.add(None)
                    continue
                corner = list(a)
                corner[differ[VIA]] = b[differ[VIA]]
                at = [r for r in range(south) if list(lines[r, line].coords) == corner]
                choices.add(at[0] if at else None)
            if len(choices) == 1 and None not in choices:
                found[p, side] = choices.pop()
    fits = all(abs(r - (p - 1 if side == 0 else p + 1)) == 1 for (p, side), r in found.items())
    if len(set(found.values())) != len(found) or not fits:
        return {}
    return found


def kernel(
    sizes, relays, u_hbm, e_hbm, c_hbm, c, end, before,
    ab, z, zs, pin, sbuf,
    s_send, s_recv, d_send, d_recv, e_send, e_recv, di_recv, load_sem, *extra,
):
    rows, cols, depth, lanes = u_hbm.shape
    pieces = min(PIECES, cols)
    wide = cols // pieces
    square = is_square(sizes, relays)
    extra = list(extra)
    if relays:
        relay_buf, h_recv, h_send = extra[:3]
        del extra[:3]
    if square:
        held, q_send, q_recv = extra
    else:
        p_send, p_recv = extra
    place = {axis: lax.axis_index(axis) for axis in sizes}
    below = {axis: place[axis] > 0 for axis in sizes}
    above = {axis: place[axis] < sizes[axis] - 1 for axis in sizes}
    scale = 1.0 / (rows * sizes["south"])

    odd = lax.rem(place["east"], 2) == 1

    def piece(n):
        return jnp.where(odd, n, pieces - 1 - n)

    def target(axis, side):
        step = sizes[axis] - 1 if side == 0 else 1
        return {axis: lax.rem(place[axis] + step, sizes[axis])}

    def sends(axis, side):
        return below[axis] if side == 0 else above[axis]

    def receives(axis, side):
        return above[axis] if side == 0 else below[axis]

    def remote(src, dst, send, recv, axis, side):
        return pltpu.make_async_remote_copy(
            src_ref=src, dst_ref=dst, send_sem=send, recv_sem=recv,
            device_id=target(axis, side), device_id_type=MESH,
        )

    def south(slot, side, n, first=False):
        here = (1, rows)[side]
        there = (rows + 1, 0)[side]
        src = (
            u_hbm.at[here - 1, pl.ds(n * wide, wide)]
            if first else ab.at[slot, here, pl.ds(n * wide + 1, wide)]
        )
        return remote(
            src, ab.at[slot, there, pl.ds(n * wide + 1, wide)],
            s_send.at[slot, side], s_recv.at[slot, side, n], "south", side,
        )

    def south_sent(slot, side):
        row = ab.at[slot, (1, rows)[side], pl.ds(1, cols)]
        return remote(
            row, row, s_send.at[slot, side], s_recv.at[slot, side, 0], "south", side
        )

    def down(slot, side):
        part = pl.ds(0, 2)
        return remote(
            zs.at[slot, side, part], z.at[slot, 1 - side, part],
            d_send.at[slot, side], d_recv.at[slot, side], "down", side,
        )

    def down_inner(slot, side):
        part = pl.ds(2, rows - 2)
        return remote(
            zs.at[slot, side, part], z.at[slot, 1 - side, part],
            d_send.at[slot, side], di_recv.at[slot, side], "down", side,
        )

    def down_sent(slot, side):
        return remote(
            zs.at[slot, side], z.at[slot, 1 - side],
            d_send.at[slot, side], di_recv.at[slot, side], "down", side,
        )

    def east(slot, side, first=False):
        here = (1, cols)[side]
        there = (cols + 1, 0)[side]
        own = pl.ds(1, rows)
        src = u_hbm.at[pl.ds(0, rows), here - 1] if first else ab.at[slot, own, here]
        return remote(
            src, ab.at[slot, own, there],
            e_send.at[slot, side], e_recv.at[slot, side], "east", side,
        )

    def by_place(table, other):
        value = jnp.int32(other)
        for p, entry in table.items():
            value = jnp.where(place["south"] == p, entry, value)
        return value

    relay_at = [
        by_place({p: r for (p, s), r in relays.items() if s == side}, -1) for side in (0, 1)
    ]
    served = by_place({r: p for (p, _), r in relays.items()}, -1)
    served_side = by_place({r: side for (_, side), r in relays.items()}, 0)
    is_relay = served >= 0

    def hop_in(t, slot, side, n, m, first=False):
        here = (1, rows)[side]
        src = (
            u_hbm.at[here - 1, pl.ds(n * wide, wide)]
            if first else ab.at[slot, here, pl.ds(n * wide + 1, wide)]
        )
        return pltpu.make_async_remote_copy(
            src_ref=src, dst_ref=relay_buf.at[t, m],
            send_sem=s_send.at[slot, side], recv_sem=h_recv.at[lax.rem(jnp.int32(t), 2), m],
            device_id={"south": jnp.maximum(relay_at[side], 0)}, device_id_type=MESH,
        )

    def hop_out(t, m):
        n = piece(2 * m + 1)
        slot = lax.rem(jnp.int32(t), 2)
        there = jnp.where(served_side == 0, rows + 1, 0)
        goal = served + 2 * served_side - 1
        return pltpu.make_async_remote_copy(
            src_ref=relay_buf.at[t, m],
            dst_ref=ab.at[slot, there, pl.ds(n * wide + 1, wide)],
            send_sem=h_send.at[slot], recv_sem=s_recv.at[slot, served_side, n],
            device_id={"south": jnp.maximum(goal, 0)}, device_id_type=MESH,
        )

    def hops_sent(t):
        goal = served + 2 * served_side - 1
        return pltpu.make_async_remote_copy(
            src_ref=relay_buf.at[t], dst_ref=relay_buf.at[t],
            send_sem=h_send.at[lax.rem(jnp.int32(t), 2)], recv_sem=h_recv.at[0, 0],
            device_id={"south": jnp.maximum(goal, 0)}, device_id_type=MESH,
        )

    def forward(t, m):
        if relays:
            @pl.when(is_relay)
            def _():
                @pl.when(jnp.logical_and(t >= 2, m == 0))
                def _():
                    hops_sent(t - 2).wait_send()

                hop_in(t, 0, 0, 0, m).wait_recv()
                hop_out(t, m).start()

    def send_south(t, slot, turn, first=False):
        n = piece(turn)
        for side in (0, 1):
            here = sends("south", side)
            if relays:
                bent = jnp.logical_and(relay_at[side] >= 0, lax.rem(turn, 2) == 1)

                @pl.when(jnp.logical_and(here, bent))
                def _():
                    hop_in(t, slot, side, n, turn // 2, first).start()

                here = jnp.logical_and(here, jnp.logical_not(bent))

            @pl.when(here)
            def _():
                south(slot, side, n, first).start()

    def each(act, when, axis, copy):
        for side in (0, 1):
            @pl.when(when(axis, side))
            def _():
                getattr(copy(side), act)()

    barrier = pltpu.get_barrier_semaphore()
    for axis in sizes:
        for side in (0, 1):
            @pl.when(sends(axis, side))
            def _():
                pl.semaphore_signal(
                    barrier, inc=1, device_id=target(axis, side), device_id_type=MESH
                )
    met = 0
    if relays:
        for side in (0, 1):
            @pl.when(relay_at[side] >= 0)
            def _():
                pl.semaphore_signal(
                    barrier, inc=1, device_id={"south": jnp.maximum(relay_at[side], 0)},
                    device_id_type=MESH,
                )

            met = met + (relay_at[side] >= 0).astype(jnp.int32)

        @pl.when(is_relay)
        def _():
            pl.semaphore_signal(
                barrier, inc=1, device_id={"south": jnp.maximum(served, 0)},
                device_id_type=MESH,
            )

        met = met + is_relay.astype(jnp.int32)
    for axis in sizes:
        met = met + below[axis].astype(jnp.int32) + above[axis].astype(jnp.int32)

    own = (pl.ds(1, rows), pl.ds(1, cols))
    loads = [
        pltpu.make_async_copy(u_hbm, ab.at[(0,) + own], load_sem.at[0]),
        pltpu.make_async_copy(e_hbm, ab.at[(1,) + own], load_sem.at[1]),
        pltpu.make_async_copy(c_hbm, c, load_sem.at[2]),
    ]
    loads[0].start()
    pl.semaphore_wait(barrier, met)

    @pl.loop(0, pieces)
    def _(n):
        send_south(0, 0, n, True)

    each("start", sends, "east", lambda side: east(0, side, True))
    loads[1].start()
    loads[2].start()

    blank = jnp.zeros((depth, lanes), jnp.float32)
    for side, missing in ((0, below), (1, above)):
        @pl.when(jnp.logical_not(missing["south"]))
        def _():
            @pl.loop(0, cols)
            def _(i):
                for slot in (0, 1):
                    ab[slot, (0, rows + 1)[side], i + 1] = blank

        @pl.when(jnp.logical_not(missing["east"]))
        def _():
            @pl.loop(0, rows)
            def _(j):
                for slot in (0, 1):
                    ab[slot, j + 1, (0, cols + 1)[side]] = blank

        @pl.when(jnp.logical_not(missing["down"]))
        def _():
            @pl.loop(0, cols)
            def _(i):
                for slot in (0, 1):
                    for r in range(rows):
                        z[slot, side, r, i] = blank[:1]

    loads[0].wait()

    @pl.loop(0, cols)
    def _(i):
        for r in range(rows):
            j = 0 if r == 0 else rows - 1 if r == 1 else r - 1
            zs[0, 0, r, i] = ab[0, j + 1, i + 1, pl.ds(0, 1)]
            zs[0, 1, r, i] = ab[0, j + 1, i + 1, pl.ds(depth - 1, 1)]

    each("start", sends, "down", lambda side: down(0, side))
    each("start", sends, "down", lambda side: down_inner(0, side))
    loads[1].wait()
    loads[2].wait()

    for m in range(pieces // 2):
        forward(0, m)

    level = lax.broadcasted_iota(jnp.int32, (depth, lanes), 0)

    def cell(now, later, j, i, r, final=False):
        x = ab[now, j + 1, i + 1]
        lower = jnp.where(level == 0, z[now, 0, r, i], pltpu.roll(x, 1, 0))
        upper = jnp.where(level == depth - 1, z[now, 1, r, i], pltpu.roll(x, depth - 1, 0))
        spread = (
            ab[now, j, i + 1] + ab[now, j + 2, i + 1]
            + ab[now, j + 1, i] + ab[now, j + 1, i + 2]
            + lower + upper - 6.0 * x
        )
        new = 2.0 * x - ab[later, j + 1, i + 1] + c[j, i] * spread
        if final:
            end[j, i] = new
            return
        ab[later, j + 1, i + 1] = new
        zs[later, 0, r, i] = new[:1]
        zs[later, 1, r, i] = new[depth - 1:]

    def inner(step, now, later, final=False):
        each("wait_recv", receives, "east", lambda side: east(now, side))
        each("wait_recv", receives, "down", lambda side: down_inner(now, side))

        @pl.when(step >= 1)
        def _():
            each("wait_send", sends, "east", lambda side: east(later, side))
            each("wait_send", sends, "down", lambda side: down_sent(later, side))
            each("wait_send", sends, "south", lambda side: south_sent(later, side))

        @pl.loop(1, rows - 1)
        def _(j):
            @pl.loop(0, cols)
            def _(i):
                cell(now, later, j, i, j + 1, final)

        @pl.when(step < STEPS - 1)
        def _():
            each("start", sends, "down", lambda side: down_inner(later, side))

    def edges_sent(slot, n):
        for side in (0, 1):
            @pl.when(jnp.logical_and(sends("east", side), n == (0, pieces - 1)[side]))
            def _():
                east(slot, side).start()

    def outer_piece(step, now, later, turn, final=False):
        n = piece(turn)
        each("wait_recv", receives, "south", lambda side: south(now, side, n))

        @pl.when(turn == 0)
        def _():
            each("wait_recv", receives, "down", lambda side: down(now, side))

        @pl.loop(0, wide)
        def _(w):
            i = n * wide + w
            cell(now, later, 0, i, 0, final)
            cell(now, later, rows - 1, i, 1, final)

        @pl.when(step < STEPS - 1)
        def _():
            send_south(step + 1, later, turn)

            @pl.when(turn == pieces - 1)
            def _():
                each("start", sends, "down", lambda side: down(later, side))

            edges_sent(later, n)

    @pl.loop(0, STEPS - 1)
    def _(step):
        now = lax.rem(step, 2)
        inner(step, now, 1 - now)

        @pl.loop(0, pieces)
        def _(n):
            outer_piece(step, now, 1 - now, n)
            if relays:
                @pl.when(jnp.logical_and(lax.rem(n, 2) == 1, n >= 3))
                def _():
                    forward(step + 1, n // 2 - 1)

        if relays:
            forward(step + 1, pieces // 2 - 1)

    last = STEPS - 1
    now, later = last % 2, 1 - last % 2
    inner(last, now, later, True)

    def carry(n):
        return remote(
            sbuf.at[pl.ds(n * wide, wide)], pin.at[pl.ds(n * wide, wide)],
            p_send.at[0], p_recv.at[n], "south", 1,
        )

    first = jnp.logical_not(below["south"])
    spot = place["south"]

    def total_copy(n, src, dst, way, kind, goal):
        part = pl.ds(n * wide, wide)
        return pltpu.make_async_remote_copy(
            src_ref=src.at[part], dst_ref=dst.at[part],
            send_sem=q_send.at[way], recv_sem=q_recv.at[kind, n],
            device_id={"south": goal}, device_id_type=MESH,
        )

    early = pieces // 4

    def totals_sent(way, count=pieces):
        part = pl.ds(0, count * wide)
        return pltpu.make_async_remote_copy(
            src_ref=sbuf.at[part], dst_ref=pin.at[part],
            send_sem=q_send.at[way], recv_sem=q_recv.at[0, 0],
            device_id={"south": lax.rem(spot + 1, 4)}, device_id_type=MESH,
        )

    def beside(n):
        return total_copy(n, sbuf, pin, 0, 0, lax.rem(spot + 1, 4))

    def across(n):
        return total_copy(n, sbuf, pin, 1, 0, 2)

    def upward(n):
        return total_copy(n, sbuf, held, 1, 1, 3)

    def direct(n):
        return total_copy(n, sbuf, held, 0, 1, 2)

    def onward(n):
        return total_copy(n, held, held, 1, 1, 2)

    def middle_total(turn):
        n = piece(turn)

        @pl.when(spot == 2)
        def _():
            beside(n).wait_recv()

            @pl.loop(0, wide)
            def _(w):
                i = n * wide + w
                sbuf[i] = pin[i] + c[rows - 1, i]

            beside(n).start()

        @pl.when(spot == 3)
        def _():
            upward(n).wait_recv()

            @pl.when(turn >= early)
            def _():
                onward(n).start()

    @pl.loop(0, pieces)
    def _(turn):
        n = piece(turn)
        outer_piece(last, now, later, turn, True)

        @pl.loop(0, wide)
        def _(w):
            i = n * wide + w
            sum_here = jnp.zeros((depth, lanes), jnp.float32)
            for j in range(rows):
                sum_here = sum_here + end[j, i]
                c[j, i] = sum_here * scale

        if square:
            @pl.when(spot < 2)
            def _():
                @pl.loop(0, wide)
                def _(w):
                    i = n * wide + w
                    sbuf[i] = c[rows - 1, i]

            @pl.when(spot == 0)
            def _():
                beside(n).start()
                across(n).start()

            @pl.when(spot == 1)
            def _():
                upward(n).start()

                @pl.when(turn < early)
                def _():
                    direct(n).start()

            @pl.when(turn >= 2)
            def _():
                middle_total(turn - 2)
        else:
            @pl.when(first)
            def _():
                @pl.loop(0, wide)
                def _(w):
                    i = n * wide + w
                    sbuf[i] = c[rows - 1, i]

                @pl.when(above["south"])
                def _():
                    carry(n).start()

    @pl.when(first)
    def _():
        @pl.loop(0, cols)
        def _(i):
            before[i] = blank

    if square:
        @pl.loop(pieces - 2, pieces)
        def _(turn):
            middle_total(turn)

    if relays:
        @pl.when(is_relay)
        def _():
            for t in range(max(STEPS - 2, 0), STEPS):
                hops_sent(t).wait_send()

    each("wait_send", sends, "east", lambda side: east(now, side))
    each("wait_send", sends, "down", lambda side: down_sent(now, side))
    each("wait_send", sends, "south", lambda side: south_sent(now, side))

    if square:
        @pl.when(spot == 1)
        def _():
            @pl.loop(0, pieces)
            def _(turn):
                n = piece(turn)
                beside(n).wait_recv()

                @pl.loop(0, wide)
                def _(w):
                    i = n * wide + w
                    before[i] = pin[i]

        @pl.when(spot >= 2)
        def _():
            @pl.loop(0, pieces)
            def _(turn):
                n = piece(turn)

                @pl.when(spot == 2)
                def _():
                    upward(n).wait_recv()

                @pl.when(spot == 3)
                def _():
                    beside(n).wait_recv()

                @pl.loop(0, wide)
                def _(w):
                    i = n * wide + w
                    before[i] = pin[i] + held[i]
    else:
        @pl.when(below["south"])
        def _():
            @pl.loop(0, pieces)
            def _(turn):
                n = piece(turn)
                carry(n).wait_recv()

                @pl.loop(0, wide)
                def _(w):
                    i = n * wide + w
                    sbuf[i] = c[rows - 1, i] + pin[i]
                    before[i] = pin[i]

                @pl.when(above["south"])
                def _():
                    carry(n).start()

    if square:
        @pl.when(lax.rem(spot, 2) == 0)
        def _():
            totals_sent(0).wait_send()

        @pl.when(spot < 2)
        def _():
            totals_sent(1).wait_send()

        if early:
            @pl.when(spot == 1)
            def _():
                totals_sent(0, early).wait_send()

        @pl.when(spot == 3)
        def _():
            totals_sent(1, pieces - early).wait_send()
    else:
        @pl.when(above["south"])
        def _():
            remote(sbuf, pin, p_send.at[0], p_recv.at[0], "south", 1).wait_send()


def writer(part, end, before, total_hbm, end_hbm, total, sem):
    rows, cols = part.shape[:2]
    for j in range(rows):
        pltpu.make_async_copy(end.at[j], end_hbm.at[j], sem.at[0]).start()
    for j in range(rows):
        @pl.loop(0, cols)
        def _(i):
            total[j, i] = part[j, i] + before[i]

        pltpu.make_async_copy(total.at[j], total_hbm.at[j], sem.at[1]).start()
    pltpu.make_async_copy(end, end_hbm, sem.at[0]).wait()
    pltpu.make_async_copy(total, total_hbm, sem.at[1]).wait()


def is_square(sizes, relays):
    return sizes["south"] == 4 and relays == {(2, 0): 0, (1, 1): 3}


def shards(sizes, relays, field_now, earlier, speed_square):
    rows, cols, depth, lanes = field_now.shape
    pieces = min(PIECES, cols)
    relays = relays if pieces % 2 == 0 else {}
    edge = (2, 2, rows, cols, 1, lanes)
    dma = pltpu.SemaphoreType.DMA
    anywhere = pl.BlockSpec(memory_space=pltpu.HBM)
    inside = pl.BlockSpec(memory_space=pltpu.VMEM)
    part, end, before = pl.pallas_call(
        functools.partial(kernel, sizes, relays),
        out_shape=(
            pltpu.VMEM(field_now.shape, jnp.float32),
            pltpu.VMEM(field_now.shape, jnp.float32),
            pltpu.VMEM((cols, depth, lanes), jnp.float32),
        ),
        in_specs=[anywhere] * 3,
        out_specs=(inside,) * 3,
        scratch_shapes=[
            pltpu.VMEM((2, rows + 2, cols + 2, depth, lanes), jnp.float32),
            pltpu.VMEM(edge, jnp.float32),
            pltpu.VMEM(edge, jnp.float32),
            pltpu.VMEM((cols, depth, lanes), jnp.float32),
            pltpu.VMEM((cols, depth, lanes), jnp.float32),
            dma((2, 2)), dma((2, 2, pieces)), dma((2, 2)), dma((2, 2)),
            dma((2, 2)), dma((2, 2)), dma((2, 2)), dma((3,)),
        ] + ([
            pltpu.VMEM((STEPS, pieces // 2, cols // pieces, depth, lanes), jnp.float32),
            dma((2, pieces // 2)), dma((2,)),
        ] if relays else []) + ([
            pltpu.VMEM((cols, depth, lanes), jnp.float32), dma((2,)), dma((2, pieces)),
        ] if is_square(sizes, relays) else [dma((1,)), dma((pieces,))]),
        compiler_params=pltpu.CompilerParams(
            collective_id=0, has_side_effects=True, vmem_limit_bytes=VMEM_LIMIT
        ),
        name="wave",
    )(field_now, earlier, speed_square)
    return pl.pallas_call(
        writer,
        out_shape=(jax.ShapeDtypeStruct(field_now.shape, jnp.float32),) * 2,
        in_specs=[inside] * 3,
        out_specs=(anywhere,) * 2,
        scratch_shapes=[pltpu.VMEM(field_now.shape, jnp.float32), dma((2,))],
        compiler_params=pltpu.CompilerParams(vmem_limit_bytes=WRITER_LIMIT),
        name="write",
    )(part, end, before)


def solution(mesh):
    placed = P("south", "east", "down", None)
    sizes = {axis: mesh.shape[axis] for axis in ("south", "east", "down")}
    relays = corner_relays(mesh)
    return jax.shard_map(
        functools.partial(shards, sizes, relays),
        mesh=mesh,
        in_specs=(placed,) * 3,
        out_specs=(placed,) * 2,
        check_vma=False,
    )
```
